256 devices in a mesh: gx: 8 (over x, z_lo), gy: 8 (over z_hi, core), ha: 4 (over y).
Axes of the slice: x: 4, y: 4, z: 8 (z_hi: 4, z_lo: 2; z = z_hi * 2 + z_lo), core: 2. Of those that a mesh axis runs over, the one named last changes fastest.
Arguments:
- density: bfloat16 [3, 625, 8, 8, 1024], P(None, None, 'gx', 'gy', 'ha'), may hold values from -6 to 6
- upsample: bfloat16 [2112, 625], replicated, may hold values from -0.25 to 0.25
- normal_kernel: bfloat16 [625, 2112], replicated, may hold values from -0.125 to 0.125
- tangent_kernel: bfloat16 [625, 2112], replicated, may hold values from -0.125 to 0.125
- self_operator: bfloat16 [625, 625], replicated, may hold values from -0.25 to 0.25
- rim_list: int32 [8, 8, 128], P('gx', 'gy', 'ha'), may hold values from 0 to 255
- pair_target: int32 [8, 8, 4, 256], P('gx', 'gy', 'ha'), may hold values from 0 to 1023
- pair_source: int32 [8, 8, 4, 256], P('gx', 'gy', 'ha'), may hold values from 0 to 2175
- pair_weight: float32 [8, 8, 4, 256], P('gx', 'gy', 'ha'), may hold values from 0.5 to 2
- pair_angles: float32 [3, 8, 8, 4, 256], P(None, 'gx', 'gy', 'ha'), may hold values from -3.140625 to 3.140625
- live_count: int32 [8, 8, 4], P('gx', 'gy', 'ha'), may hold values from 1 to 256, as said below
Outputs:
- induced: float32 [3, 625, 8, 8, 1024], P(None, None, 'gx', 'gy', 'ha')
The draws below stay inside these ranges and needn't reach their ends.
Inputs may be any that keep to these rules, and one draw needn't show every extreme that they name: `rim_list`: an index into the device's own 256 grains. `pair_target`: an index into the 1024 grains of the pair's slab. `pair_source`: an index into the slab's source pool. `live_count`: some device uses all 256 slots.
All inputs are finite; a program needn't handle non-finite values.
Results may differ from the reference program's by a relative error of at most 0.0024.
Values may be sent and summed in bfloat16 or wider, within the bound.
A program may use at most 128 MiB of HBM per device.

```python
import math
import jax
import jax.numpy as jnp
from jax import lax

COEFFS = 625
NODES = 2112
GRAINS_DEV = 256
RIM = 32
SLOTS = 256
SLAB_GRAINS = 1024
RIM_SLAB = 128
POOL = 2176
N_GX = 8
N_GY = 8
N_HA = 4


def draw_live_count(key, part):
    first_key, second_key, third_key, fourth_key = jax.random.split(jax.random.fold_in(key, 17), 4)
    dense = jax.random.randint(first_key, (N_GX, N_GY, 1), 0, 4) == 0
    higher = jax.random.randint(second_key, (N_GX, N_GY, N_HA), 2 * SLOTS // 3, SLOTS + 1)
    lower = jax.random.randint(third_key, (N_GX, N_GY, N_HA), max(SLOTS // 8, 1), SLOTS // 4 + 1)
    counts = jnp.where(dense, higher, lower).reshape(-1)
    chosen = jax.random.randint(fourth_key, (), 0, N_GX * N_GY * N_HA)
    counts = jnp.where(jnp.arange(counts.shape[0]) == chosen, SLOTS, counts)
    return counts.reshape(N_GX, N_GY, N_HA).astype(jnp.int32)


def touch_ends(drawn, key, low, largest):
    longest = drawn.shape.index(max(drawn.shape))
    spots = []
    for shift in (0, 1):
        where = [jax.random.randint(jax.random.fold_in(key, axis), (), 0, length) for axis, length in enumerate(drawn.shape)]
        where[longest] = (where[longest] + shift) % drawn.shape[longest]
        spots.append(tuple(where))
    return drawn.at[spots[0]].set(low).at[spots[1]].set(largest)


def block_scale(stream_key, extent, cuts, smallest, high):
    level, own = 1.0, jax.random.fold_in(stream_key, 6)
    for position, blocks in cuts:
        heights = jnp.exp(jax.random.uniform(jax.random.fold_in(own, position), (blocks,), jnp.float32, smallest / len(cuts), high / len(cuts)))
        level = level * jnp.repeat(heights, extent[position] // blocks).reshape([-1 if axis == position else 1 for axis in range(len(extent))])
    return level


def gaussian(key, extent, scale, limit, pieces=(), held_as=jnp.bfloat16):
    result = scale * jax.random.normal(key, extent, jnp.float32)
    if pieces:
        result = result * block_scale(key, extent, pieces, -0.22, 0.18)
    return jnp.clip(result, -limit, limit).astype(held_as)


def setup_inputs(seed: int = 0) -> dict:
    splits = jax.random.split(jax.random.key(seed), 12)
    density = gaussian(splits[0], (3, COEFFS, N_GX, N_GY, SLAB_GRAINS), 1.0, 6.0, ((2, 8), (3, 8), (4, 4)))
    upsample = gaussian(splits[1], (NODES, COEFFS), COEFFS ** -0.5, 0.25)
    normal_kernel = gaussian(splits[2], (COEFFS, NODES), NODES ** -0.5, 0.125)
    tangent_kernel = gaussian(splits[3], (COEFFS, NODES), NODES ** -0.5, 0.125)
    self_operator = gaussian(splits[4], (COEFFS, COEFFS), COEFFS ** -0.5, 0.25)
    rim_list = touch_ends(jax.random.randint(splits[5], (N_GX, N_GY, RIM_SLAB), 0, GRAINS_DEV), jax.random.fold_in(splits[5], 1), 0, GRAINS_DEV - 1).astype(jnp.int32)
    pair_target = touch_ends(jax.random.randint(splits[6], (N_GX, N_GY, N_HA, SLOTS), 0, SLAB_GRAINS), jax.random.fold_in(splits[6], 1), 0, SLAB_GRAINS - 1).astype(jnp.int32)
    pair_source = touch_ends(jax.random.randint(splits[7], (N_GX, N_GY, N_HA, SLOTS), 0, POOL), jax.random.fold_in(splits[7], 1), 0, POOL - 1).astype(jnp.int32)
    pair_weight = jnp.clip(jnp.exp(math.log(2.0) - 1.3862944 * jax.random.uniform(splits[8], (N_GX, N_GY, N_HA, SLOTS), jnp.float32) ** block_scale(splits[8], (N_GX, N_GY, N_HA, SLOTS), ((0, 8), (1, 8), (2, 4)), -0.2, 0.2)), 0.5, 2.0)
    pair_angles = jnp.clip(jax.random.uniform(splits[9], (3, N_GX, N_GY, N_HA, SLOTS), jnp.float32, -3.140625, 3.140625), -3.140625, 3.140625)
    live_count = draw_live_count(jax.random.fold_in(splits[11], 71), 0)
    return dict(density=density, upsample=upsample, normal_kernel=normal_kernel, tangent_kernel=tangent_kernel, self_operator=self_operator, rim_list=rim_list, pair_target=pair_target, pair_source=pair_source, pair_weight=pair_weight, pair_angles=pair_angles, live_count=live_count)


def rotation(angles):
    first, second, third = angles[0], angles[1], angles[2]
    all_zeros = jnp.zeros_like(first)
    all_ones = jnp.ones_like(first)

    def about_z(angle_value):
        cosine, sine_value = jnp.cos(angle_value), jnp.sin(angle_value)
        return jnp.stack([jnp.stack([cosine, -sine_value, all_zeros]), jnp.stack([sine_value, cosine, all_zeros]), jnp.stack([all_zeros, all_zeros, all_ones])])

    cosine, sine_value = jnp.cos(second), jnp.sin(second)
    tilt = jnp.stack([jnp.stack([cosine, all_zeros, sine_value]), jnp.stack([all_zeros, all_ones, all_zeros]), jnp.stack([-sine_value, all_zeros, cosine])])
    return jnp.einsum("abp,bcp,cdp->adp", about_z(first), tilt, about_z(third), precision=lax.Precision.HIGHEST)


def reference(density, upsample, normal_kernel, tangent_kernel, self_operator, rim_list, pair_target, pair_source, pair_weight, pair_angles, live_count):
    slab_total = N_GX * N_GY
    flattened = density.reshape(3, COEFFS, slab_total, SLAB_GRAINS)
    listed = rim_list.reshape(slab_total, N_HA, RIM) + (jnp.arange(N_HA, dtype=jnp.int32) * GRAINS_DEV)[None, :, None]
    listed = listed.reshape(slab_total, RIM_SLAB).astype(jnp.int32)
    targets_all = pair_target.reshape(slab_total, N_HA * SLOTS)
    sources_all = pair_source.reshape(slab_total, N_HA * SLOTS)
    weights_all = pair_weight.reshape(slab_total, N_HA * SLOTS)
    angles_all = pair_angles.reshape(3, slab_total, N_HA * SLOTS)
    counts_all = live_count.reshape(slab_total, N_HA)
    up_wide = upsample.astype(jnp.float32)
    normal_wide = normal_kernel.astype(jnp.float32)
    tangent_wide = tangent_kernel.astype(jnp.float32)
    self_wide = self_operator.astype(jnp.float32)

    def one_slab(slab_index):
        slab_row = slab_index // N_GY
        column = slab_index % N_GY
        offsets = jnp.arange(3, dtype=jnp.int32) - 1
        near_rows = (slab_row + offsets) % N_GX
        near_cols = (column + offsets) % N_GY
        nearby = (near_rows[:, None] * N_GY + near_cols[None, :]).reshape(9).astype(jnp.int32)
        owned = jnp.take(flattened, slab_index, axis=2)
        beside_all = jnp.take(flattened, nearby, axis=2)
        rim_index = jnp.take(listed, nearby, axis=0)
        rimset = jnp.take_along_axis(beside_all, rim_index[None, None], axis=3).reshape(3, COEFFS, 9 * RIM_SLAB)
        source_pool = jnp.concatenate([owned, rimset], axis=2)
        source = jnp.take(sources_all, slab_index, axis=0)
        target = jnp.take(targets_all, slab_index, axis=0)
        weight = jnp.take(weights_all, slab_index, axis=0)
        angles = jnp.take(angles_all, slab_index, axis=1)
        counts = jnp.take(counts_all, slab_index, axis=0)
        alive_mask = (jnp.arange(SLOTS, dtype=jnp.int32)[None, :] < counts[:, None]).reshape(-1)
        scaling = jnp.where(alive_mask, weight, jnp.float32(0.0))
        picked = jnp.take(source_pool, source, axis=2)
        node_values = jnp.einsum("qk,ckp->cqp", up_wide, picked.astype(jnp.float32)).astype(jnp.bfloat16)
        frames = rotation(angles)
        node_wide = node_values.astype(jnp.float32)
        rotated = (frames[:, 0, None, :] * node_wide[0] + frames[:, 1, None, :] * node_wide[1] + frames[:, 2, None, :] * node_wide[2]).astype(jnp.bfloat16)
        rotated_wide = rotated.astype(jnp.float32)
        quad_normal = jnp.einsum("kq,qp->kp", normal_wide, rotated_wide[0])
        quad_tangent = jnp.einsum("kq,cqp->ckp", tangent_wide, rotated_wide[1:])
        quad = jnp.concatenate([quad_normal[None], quad_tangent], axis=0)
        contribution = (frames[0, :, None, :] * quad[0] + frames[1, :, None, :] * quad[1] + frames[2, :, None, :] * quad[2]) * scaling[None, None, :]
        summed = jnp.zeros((3, COEFFS, SLAB_GRAINS), jnp.float32).at[:, :, target].add(contribution)
        self_term = jnp.einsum("jk,ckg->cjg", self_wide, owned.astype(jnp.float32))
        return summed + self_term

    results = lax.map(one_slab, jnp.arange(slab_total, dtype=jnp.int32))
    return jnp.transpose(results, (1, 2, 0, 3)).reshape(3, COEFFS, N_GX, N_GY, SLAB_GRAINS)
```

```python
import functools

import jax
import jax.numpy as jnp
from jax import lax
from jax.experimental import pallas as pl
from jax.experimental.pallas import tpu as pltpu
from jax.sharding import PartitionSpec as P

MESH = pl.DeviceIdType.MESH
ANY = pl.BlockSpec(memory_space=pl.ANY)
VMEM = pl.BlockSpec(memory_space=pltpu.VMEM)
SMEM = pl.BlockSpec(memory_space=pltpu.SMEM)
CAPACITY = 96
TABLE = 16
SCALE, SOURCE_PLACE, SOURCE_COLUMN, TARGET_PLACE, TARGET_COLUMN = 9, 10, 11, 12, 13
NT = (((1,), (1,)), ((), ()))
TN = (((0,), (0,)), ((), ()))
F32 = jnp.float32
BF16 = jnp.bfloat16


def padded(width):
    return (width + 127) // 128 * 128


def local_params():
    return pltpu.CompilerParams(vmem_limit_bytes=58 * 1024 * 1024)


def pair_table(angles, weight, source, target, live, grains, rim, places):
    c0, c1, c2 = (jnp.cos(angles[i]) for i in range(3))
    s0, s1, s2 = (jnp.sin(angles[i]) for i in range(3))
    frame = [
        c0 * c1 * c2 - s0 * s2, -(c0 * c1 * s2) - s0 * c2, c0 * s1,
        s0 * c1 * c2 + c0 * s2, -(s0 * c1 * s2) + c0 * c2, s0 * s1,
        -(s1 * c2), s1 * s2, c1,
    ]
    slots = source.shape[0]
    alive = jnp.arange(slots, dtype=jnp.int32) < live
    scaling = jnp.where(alive, weight, F32(0.0))
    inside = source < grains * places
    listed = jnp.maximum(source - grains * places, 0)
    group, within = listed // (rim * places), listed % (rim * places)
    source_place = jnp.where(inside, source // grains, within // rim)
    source_column = jnp.where(inside, source % grains, grains + group * rim + within % rim)
    target_place = jnp.where(alive, target // grains, -1)
    rows = frame + [scaling, source_place, source_column, target_place, target % grains]
    rows = [row.astype(F32) for row in rows] + [jnp.zeros((slots,), F32)] * (TABLE - len(rows))
    return jnp.stack(rows)


def rim_kernel(list_ref, own_ref, out_ref):
    rim, grains = list_ref.shape[0], own_ref.shape[2]
    width = own_ref.shape[1]
    step = padded(width)
    lanes = lax.broadcasted_iota(jnp.int32, (rim, grains), 1)
    pick = jnp.where(list_ref[...] == lanes, 1.0, 0.0).astype(BF16)
    out_ref[...] = jnp.zeros_like(out_ref)
    for c in range(3):
        found = lax.dot_general(pick, own_ref[c], NT, preferred_element_type=F32)
        out_ref[:, c * step : c * step + width] = found.astype(BF16)


def halo_kernel(sizes, rim_ref, table_ref, rims_ref, tables_ref, send_sem, recv_sem, own_sem):
    n_gx, n_gy, n_ha = sizes
    x, y, h = lax.axis_index("gx"), lax.axis_index("gy"), lax.axis_index("ha")
    beside = [(dx, dy) for dx in (-1, 0, 1) for dy in (-1, 0, 1) if (dx, dy) != (0, 0)]
    sends = []
    for dx, dy in beside:
        device = (lax.rem(x + dx + n_gx, n_gx), lax.rem(y + dy + n_gy, n_gy), h)
        slot = (1 - dx) * 3 + 1 - dy
        sends.append((device, rim_ref, rims_ref.at[slot], slot))
    for j in range(1, n_ha):
        device = (x, y, lax.rem(h + j, n_ha))
        sends.append((device, table_ref, tables_ref.at[h], 9 + j))
    barrier = pltpu.get_barrier_semaphore()
    for device, _, _, _ in sends:
        pl.semaphore_signal(barrier, inc=1, device_id=device, device_id_type=MESH)
    own = [
        pltpu.make_async_copy(rim_ref, rims_ref.at[4], own_sem.at[0]),
        pltpu.make_async_copy(table_ref, tables_ref.at[h], own_sem.at[1]),
    ]
    for copy in own:
        copy.start()
    pl.semaphore_wait(barrier, len(sends))
    copies = []
    for device, source, landing, slot in sends[::-1]:
        copy = pltpu.make_async_remote_copy(
            src_ref=source,
            dst_ref=landing,
            send_sem=send_sem.at[slot],
            recv_sem=recv_sem.at[slot],
            device_id=device,
            device_id_type=MESH,
        )
        copy.start()
        copies.append(copy)
    for copy in own:
        copy.wait()
    for copy in copies:
        copy.wait()


def ranks(mask):
    total, length = mask, mask.shape[1]
    lanes = lax.broadcasted_iota(jnp.int32, mask.shape, 1)
    step = 1
    while step < length:
        total = total + jnp.where(lanes >= step, pltpu.roll(total, step, 1), 0.0)
        step *= 2
    return total - mask


def table_row(tables_ref, row):
    return jnp.concatenate([tables_ref[j, row : row + 1, :] for j in range(tables_ref.shape[0])], axis=1)


def chosen(from_place, to_place, source, target, first, count):
    mask = jnp.where((from_place == source) & (to_place == target), 1.0, 0.0)
    key = jnp.where(mask > 0.0, ranks(mask) - first, -1.0)
    rows = lax.broadcasted_iota(jnp.int32, (count, mask.shape[1]), 0).astype(F32)
    return jnp.where(rows == key, 1.0, 0.0)


def route_kernel(round_ref, place_ref, tables_ref, own_ref, rims_ref, send_ref, mine_ref, most_ref):
    places = tables_ref.shape[0]
    width, grains = own_ref.shape[1:]
    count = mine_ref.shape[0]
    step = padded(width)
    first = (round_ref[0] * count).astype(F32)
    place = place_ref[0]
    here = place.astype(F32)
    from_place, to_place = table_row(tables_ref, SOURCE_PLACE), table_row(tables_ref, TARGET_PLACE)
    column_row = table_row(tables_ref, SOURCE_COLUMN) + 1.0
    own_lanes = lax.broadcasted_iota(jnp.int32, (count, grains), 1).astype(F32)
    rim_lanes = lax.broadcasted_iota(jnp.int32, (count, rims_ref.shape[0]), 1).astype(F32) + float(grains)
    for j in range(places):
        there = lax.rem(place + j, places).astype(F32)
        select = chosen(from_place, to_place, here, there, first, count)
        column = jnp.sum(select * column_row, axis=1, keepdims=True) - 1.0
        own_pick = jnp.where(own_lanes == column, 1.0, 0.0).astype(BF16)
        rim_pick = jnp.where(rim_lanes == column, 1.0, 0.0).astype(BF16)
        out = mine_ref if j == 0 else send_ref.at[j - 1]
        for c in range(3):
            a = lax.dot_general(own_pick, own_ref[c], NT, preferred_element_type=F32)
            b = jnp.dot(rim_pick, rims_ref[:, c * step : (c + 1) * step], preferred_element_type=F32)
            out[:, c * step : (c + 1) * step] = b.astype(BF16)
            out[:, c * step : c * step + width] = (a + b[:, :width]).astype(BF16)
    most = jnp.zeros((1, 1), F32)
    for source in range(places):
        for target in range(places):
            hit = jnp.where((from_place == float(source)) & (to_place == float(target)), 1.0, 0.0)
            most = jnp.maximum(most, jnp.sum(hit, axis=1, keepdims=True))
    most_ref[...] = jnp.broadcast_to(most, most_ref.shape)


def exchange_kernel(n_ha, send_ref, recv_ref, relay_ref, send_sem, recv_sem):
    x, y, h = lax.axis_index("gx"), lax.axis_index("gy"), lax.axis_index("ha")
    right, left = (x, y, lax.rem(h + 1, n_ha)), (x, y, lax.rem(h + n_ha - 1, n_ha))
    half = send_ref.shape[1] // 2
    upper, lower = pl.ds(0, half), pl.ds(half, half)
    barrier = pltpu.get_barrier_semaphore()
    for device in (right, left):
        pl.semaphore_signal(barrier, inc=1, device_id=device, device_id_type=MESH)
    pl.semaphore_wait(barrier, 2)

    def send(source, landing, device, slot):
        copy = pltpu.make_async_remote_copy(
            src_ref=source,
            dst_ref=landing,
            send_sem=send_sem.at[slot],
            recv_sem=recv_sem.at[slot],
            device_id=device,
            device_id_type=MESH,
        )
        copy.start()
        return copy

    across = [
        send(send_ref.at[1, upper], relay_ref.at[0], right, 0),
        send(send_ref.at[1, lower], relay_ref.at[1], left, 1),
    ]
    direct = [
        send(send_ref.at[0], recv_ref.at[0], right, 2),
        send(send_ref.at[2], recv_ref.at[2], left, 3),
    ]
    across[0].wait_recv()
    onward = [send(relay_ref.at[0], recv_ref.at[1, upper], right, 4)]
    across[1].wait_recv()
    onward.append(send(relay_ref.at[1], recv_ref.at[1, lower], left, 5))
    for copy in across:
        copy.wait_send()
    for copy in direct + onward:
        copy.wait()


def apply_kernel(
    opening, round_ref, place_ref, tables_ref, mine_ref, recv_ref, upsample_ref, normal_ref, tangent_ref,
    *rest,
):
    if opening:
        self_ref, own_ref, out_ref, pick_ref, rotated_ref = rest
    else:
        before_ref, out_ref, pick_ref, rotated_ref = rest
    places = tables_ref.shape[0]
    count = mine_ref.shape[0]
    nodes, width = upsample_ref.shape
    grains = out_ref.shape[2]
    step = padded(width)
    first = (round_ref[0] * count).astype(F32)
    place = place_ref[0]
    here = place.astype(F32)
    pick_ref[:count, :] = mine_ref[...]
    pick_ref[count:, :] = recv_ref[...]
    from_place, to_place = table_row(tables_ref, SOURCE_PLACE), table_row(tables_ref, TARGET_PLACE)
    every = jnp.concatenate([tables_ref[j] for j in range(places)], axis=1)
    picked_rows = []
    for j in range(places):
        there = lax.rem(place + places - j, places).astype(F32)
        picked_rows.append(chosen(from_place, to_place, there, here, first, count))
    select = jnp.concatenate(picked_rows, axis=0)
    table = lax.dot_general(select, every, NT, precision=lax.Precision.HIGHEST, preferred_element_type=F32)
    frame = [table[:, i : i + 1] for i in range(9)]

    def evaluate(begin, size):
        values = []
        for d in range(3):
            found = lax.dot_general(
                pick_ref[:, d * step : d * step + width],
                upsample_ref[pl.ds(begin, size), :],
                NT,
                preferred_element_type=F32,
            )
            values.append(found.astype(BF16).astype(F32))
        for c in range(3):
            turned = frame[3 * c] * values[0] + frame[3 * c + 1] * values[1] + frame[3 * c + 2] * values[2]
            rotated_ref[c, :, pl.ds(begin, size)] = turned.astype(BF16)

    tile = 256
    whole = nodes // tile

    def body(i, carry):
        evaluate(pl.multiple_of(i * tile, tile), tile)
        return carry

    lax.fori_loop(0, whole, body, 0)
    if nodes % tile:
        evaluate(whole * tile, nodes % tile)
    quad = [
        jnp.dot(rotated_ref[c], (normal_ref if c == 0 else tangent_ref)[...], preferred_element_type=F32)
        for c in range(3)
    ]
    scaling = table[:, SCALE : SCALE + 1]
    lanes = lax.broadcasted_iota(jnp.int32, (places * count, grains), 1).astype(F32)
    spot = jnp.where(lanes == table[:, TARGET_COLUMN : TARGET_COLUMN + 1], 1.0, 0.0).astype(BF16)
    for c in range(3):
        given = (frame[c] * quad[0] + frame[3 + c] * quad[1] + frame[6 + c] * quad[2]) * scaling
        high = given.astype(BF16)
        low = (given - high.astype(F32)).astype(BF16)
        total = lax.dot_general(high, spot, TN, preferred_element_type=F32)
        total += lax.dot_general(low, spot, TN, preferred_element_type=F32)
        if opening:
            total += jnp.dot(self_ref[...], own_ref[c], preferred_element_type=F32)
        else:
            total += before_ref[c]
        out_ref[c] = total


def shards(
    sizes,
    density,
    upsample,
    normal_kernel,
    tangent_kernel,
    self_operator,
    rim_list,
    pair_target,
    pair_source,
    pair_weight,
    pair_angles,
    live_count,
):
    places = sizes[2]
    width, grains = density.shape[1], density.shape[4]
    nodes = upsample.shape[0]
    rim = rim_list.shape[-1]
    slots = pair_source.shape[-1]
    span = 3 * padded(width)
    count = CAPACITY
    own = density.reshape(3, width, grains)
    normal, tangent = normal_kernel.T, tangent_kernel.T
    table = pair_table(
        pair_angles.reshape(3, slots),
        pair_weight.reshape(-1),
        pair_source.reshape(-1),
        pair_target.reshape(-1),
        live_count.reshape(()),
        grains,
        rim,
        places,
    )
    listed = pl.pallas_call(
        rim_kernel,
        out_shape=jax.ShapeDtypeStruct((rim, span), BF16),
        in_specs=[VMEM, VMEM],
        out_specs=VMEM,
        compiler_params=local_params(),
        name="rims",
    )(rim_list.reshape(rim, 1), own)
    rims, tables = pl.pallas_call(
        functools.partial(halo_kernel, sizes),
        out_shape=[
            jax.ShapeDtypeStruct((9, rim, span), BF16),
            jax.ShapeDtypeStruct((places, TABLE, slots), F32),
        ],
        in_specs=[ANY, ANY],
        out_specs=[ANY, ANY],
        scratch_shapes=[
            pltpu.SemaphoreType.DMA((9 + places,)),
            pltpu.SemaphoreType.DMA((9 + places,)),
            pltpu.SemaphoreType.DMA((2,)),
        ],
        compiler_params=pltpu.CompilerParams(collective_id=0, has_side_effects=True),
        name="halo",
    )(listed, table)
    rims = rims.reshape(9 * rim, span)
    place = lax.axis_index("ha").astype(jnp.int32).reshape(1)

    def route(turn):
        return pl.pallas_call(
            route_kernel,
            out_shape=[
                jax.ShapeDtypeStruct((places - 1, count, span), BF16),
                jax.ShapeDtypeStruct((count, span), BF16),
                jax.ShapeDtypeStruct((8, 128), F32),
            ],
            in_specs=[SMEM, SMEM, VMEM, VMEM, VMEM],
            out_specs=[VMEM, VMEM, VMEM],
            compiler_params=local_params(),
            name="route",
        )(turn, place, tables, own, rims)

    def exchange(send):
        return pl.pallas_call(
            functools.partial(exchange_kernel, places),
            out_shape=jax.ShapeDtypeStruct((places - 1, count, span), BF16),
            in_specs=[ANY],
            out_specs=ANY,
            scratch_shapes=[
                pltpu.VMEM((2, count // 2, span), BF16),
                pltpu.SemaphoreType.DMA((6,)),
                pltpu.SemaphoreType.DMA((6,)),
            ],
            compiler_params=pltpu.CompilerParams(collective_id=1, has_side_effects=True),
            name="exchange",
        )(send).reshape((places - 1) * count, span)

    def apply(turn, mine, received, before):
        opening = before is None
        last = [self_operator, own] if opening else [before]
        return pl.pallas_call(
            functools.partial(apply_kernel, opening),
            out_shape=jax.ShapeDtypeStruct((3, width, grains), F32),
            in_specs=[SMEM, SMEM] + [VMEM] * (6 + len(last)),
            out_specs=VMEM,
            scratch_shapes=[
                pltpu.VMEM((places * count, span), BF16),
                pltpu.VMEM((3, places * count, nodes), BF16),
            ],
            compiler_params=local_params(),
            name="apply",
        )(turn, place, tables, mine, received, upsample, normal, tangent, *last)

    turn = jnp.zeros((1,), jnp.int32)
    send, mine, most = route(turn)
    result = apply(turn, mine, exchange(send), None)
    rounds = (most[0, 0].astype(jnp.int32) + count - 1) // count

    def again(state):
        now, total = state
        send, mine, _ = route(now.reshape(1))
        return now + 1, apply(now.reshape(1), mine, exchange(send), total)

    _, result = lax.while_loop(lambda state: state[0] < rounds, again, (jnp.int32(1), result))
    return result.reshape(3, width, 1, 1, grains)


def solution(mesh):
    sizes = tuple(mesh.shape[axis] for axis in ("gx", "gy", "ha"))
    return jax.shard_map(
        functools.partial(shards, sizes),
        mesh=mesh,
        in_specs=(
            P(None, None, "gx", "gy", "ha"),
            P(),
            P(),
            P(),
            P(),
            P("gx", "gy", "ha"),
            P("gx", "gy", "ha", None),
            P("gx", "gy", "ha", None),
            P("gx", "gy", "ha", None),
            P(None, "gx", "gy", "ha", None),
            P("gx", "gy", "ha"),
        ),
        out_specs=P(None, None, "gx", "gy", "ha"),
        check_vma=False,
    )
```

```python
import functools

import jax
import jax.numpy as jnp
from jax import lax
from jax.experimental import pallas as pl
from jax.experimental.pallas import tpu as pltpu
from jax.sharding import PartitionSpec as P

MESH = pl.DeviceIdType.MESH
ANY = pl.BlockSpec(memory_space=pl.ANY)
VMEM = pl.BlockSpec(memory_space=pltpu.VMEM)
SMEM = pl.BlockSpec(memory_space=pltpu.SMEM)
CAPACITY = 96
TABLE = 16
SCALE, SOURCE_PLACE, SOURCE_COLUMN, TARGET_PLACE, TARGET_COLUMN = 9, 10, 11, 12, 13
NT = (((1,), (1,)), ((), ()))
TN = (((0,), (0,)), ((), ()))
F32 = jnp.float32
BF16 = jnp.bfloat16


def padded(width):
    return (width + 127) // 128 * 128


def limit(mebibytes, **others):
    return pltpu.CompilerParams(vmem_limit_bytes=mebibytes * 1024 * 1024, **others)


def split(value, size):
    bits = size.bit_length() - 1
    assert size == 1 << bits
    return lax.shift_right_logical(value, bits), value & (size - 1)


def prepare_kernel(places, live_ref, list_ref, target_ref, source_ref, weight_ref, angles_ref, own_ref, rim_ref, table_ref):
    width, grains = own_ref.shape[1:]
    rim, slots = list_ref.shape[1], source_ref.shape[1]
    step = padded(width)
    square = [lax.broadcasted_iota(jnp.int32, (rim, rim), axis) for axis in (0, 1)]
    listed = jnp.where(square[0] == square[1], list_ref[...].astype(F32), 0.0)
    listed = jnp.sum(listed, axis=1, keepdims=True)
    lanes = lax.broadcasted_iota(jnp.int32, (rim, grains), 1).astype(F32)
    pick = jnp.where(listed == lanes, 1.0, 0.0).astype(BF16)
    rim_ref[...] = jnp.zeros_like(rim_ref)
    for c in range(3):
        found = lax.dot_general(pick, own_ref[c], NT, preferred_element_type=F32)
        rim_ref[:, c * step : c * step + width] = found.astype(BF16)
    c0, c1, c2 = (jnp.cos(angles_ref[i]) for i in range(3))
    s0, s1, s2 = (jnp.sin(angles_ref[i]) for i in range(3))
    frame = [
        c0 * c1 * c2 - s0 * s2, -(c0 * c1 * s2) - s0 * c2, c0 * s1,
        s0 * c1 * c2 + c0 * s2, -(s0 * c1 * s2) + c0 * c2, s0 * s1,
        -(s1 * c2), s1 * s2, c1,
    ]
    alive = lax.broadcasted_iota(jnp.int32, (1, slots), 1) < live_ref[0]
    source = source_ref[...]
    inside = source < grains * places
    place, column = split(source, grains)
    group, within = split(jnp.maximum(source - grains * places, 0), rim * places)
    rim_place, rim_column = split(within, rim)
    target_place, target_column = split(target_ref[...], grains)
    rows = frame + [
        jnp.where(alive, weight_ref[...], 0.0),
        jnp.where(inside, place, rim_place).astype(F32),
        jnp.where(inside, column, grains + group * rim + rim_column).astype(F32),
        jnp.where(alive, target_place, -1).astype(F32),
        target_column.astype(F32),
    ]
    table_ref[...] = jnp.zeros_like(table_ref)
    for i, row in enumerate(rows):
        table_ref[i : i + 1, :] = row


def gather_kernel(
    sizes, rim_ref, table_ref, own_ref, self_ref, rims_ref, tables_ref, send_ref, mine_ref, most_ref, base_ref,
    send_sem, recv_sem, own_sem,
):
    n_gx, n_gy, n_ha = sizes
    x, y, h = lax.axis_index("gx"), lax.axis_index("gy"), lax.axis_index("ha")
    near = 1 - 2 * lax.rem(y, 2)
    partner = (x, y + near, h)
    far = lax.rem(y - near + n_gy, n_gy)
    barrier = pltpu.get_barrier_semaphore()
    mates = [(x, y, lax.rem(h + j, n_ha)) for j in range(1, n_ha)]
    sides = [(lax.rem(x + dx + n_gx, n_gx), y, h) for dx in (-1, 1)]
    beyond = [(lax.rem(x + dx + n_gx, n_gx), far, h) for dx in (-1, 0, 1)]
    peers = mates + sides + beyond + [partner]
    for device in peers:
        pl.semaphore_signal(barrier, inc=1, device_id=device, device_id_type=MESH)
    own = [
        pltpu.make_async_copy(rim_ref, rims_ref.at[4], own_sem.at[0]),
        pltpu.make_async_copy(table_ref, tables_ref.at[h], own_sem.at[1]),
    ]
    for copy in own:
        copy.start()
    pl.semaphore_wait(barrier, len(peers))

    def send(source, landing, device, slot):
        copy = pltpu.make_async_remote_copy(
            src_ref=source,
            dst_ref=landing,
            send_sem=send_sem.at[slot],
            recv_sem=recv_sem.at[slot],
            device_id=device,
            device_id_type=MESH,
        )
        copy.start()
        return copy

    tables = [send(table_ref, tables_ref.at[h], mates[j], j) for j in range(n_ha - 1)]
    aside = [send(rim_ref, rims_ref.at[(1 - dx) * 3 + 1], sides[(dx + 1) // 2], n_ha + dx) for dx in (-1, 1)]
    rest = [
        send(rim_ref, rims_ref.at[(1 - dx) * 3 + 1 + near], beyond[dx + 1], n_ha + 3 + dx) for dx in (-1, 0, 1)
    ]
    rest.append(send(rim_ref, rims_ref.at[4 - near], partner, n_ha))
    for c in range(3):
        base_ref[c] = jnp.dot(self_ref[...], own_ref[c], preferred_element_type=F32)
    for copy in own:
        copy.wait()
    for copy in tables:
        copy.wait()
    columns = route_columns(jnp.float32(0.0), h, tables_ref, mine_ref.shape[0])
    outs = [mine_ref] + [send_ref.at[j] for j in range(n_ha - 1)]
    for column, out in zip(columns, outs):
        pick_own(column, own_ref, out)
    most_ref[...] = jnp.broadcast_to(longest(tables_ref), most_ref.shape)
    for i, dx in enumerate((-1, 1)):
        aside[i].wait_recv()
        rest.append(
            send(rims_ref.at[(1 - dx) * 3 + 1], rims_ref.at[(1 - dx) * 3 + 1 - near], partner, n_ha + 5 + i)
        )
    for copy in aside:
        copy.wait_send()
    for copy in rest:
        copy.wait()
    for column, out in zip(columns, outs):
        add_listed(column, rims_ref, own_ref.shape[2], out)


def ranks(mask):
    total, length = mask, mask.shape[1]
    lanes = lax.broadcasted_iota(jnp.int32, mask.shape, 1)
    step = 1
    while step < length:
        total = total + jnp.where(lanes >= step, pltpu.roll(total, step, 1), 0.0)
        step *= 2
    return total - mask


def table_row(tables_ref, row):
    return jnp.concatenate([tables_ref[j, row : row + 1, :] for j in range(tables_ref.shape[0])], axis=1)


def chosen(from_place, to_place, source, target, first, count):
    mask = jnp.where((from_place == source) & (to_place == target), 1.0, 0.0)
    key = jnp.where(mask > 0.0, ranks(mask) - first, -1.0)
    rows = lax.broadcasted_iota(jnp.int32, (count, mask.shape[1]), 0).astype(F32)
    return jnp.where(rows == key, 1.0, 0.0)


def route_columns(first, place, tables_ref, count):
    places = tables_ref.shape[0]
    here = place.astype(F32)
    from_place, to_place = table_row(tables_ref, SOURCE_PLACE), table_row(tables_ref, TARGET_PLACE)
    column_row = table_row(tables_ref, SOURCE_COLUMN) + 1.0
    columns = []
    for j in range(places):
        there = lax.rem(place + j, places).astype(F32)
        select = chosen(from_place, to_place, here, there, first, count)
        columns.append(jnp.sum(select * column_row, axis=1, keepdims=True) - 1.0)
    return columns


def longest(tables_ref):
    places = tables_ref.shape[0]
    from_place, to_place = table_row(tables_ref, SOURCE_PLACE), table_row(tables_ref, TARGET_PLACE)
    most = jnp.zeros((1, 1), F32)
    for source in range(places):
        for target in range(places):
            hit = jnp.where((from_place == float(source)) & (to_place == float(target)), 1.0, 0.0)
            most = jnp.maximum(most, jnp.sum(hit, axis=1, keepdims=True))
    return most


def pick_own(column, own_ref, out):
    count, (width, grains) = column.shape[0], own_ref.shape[1:]
    step = padded(width)
    lanes = lax.broadcasted_iota(jnp.int32, (count, grains), 1).astype(F32)
    pick = jnp.where(lanes == column, 1.0, 0.0).astype(BF16)
    out[...] = jnp.zeros(out.shape, BF16)
    for c in range(3):
        found = lax.dot_general(pick, own_ref[c], NT, preferred_element_type=F32)
        out[:, c * step : c * step + width] = found.astype(BF16)


def add_listed(column, rims_ref, grains, out):
    count, groups, rim = column.shape[0], rims_ref.shape[0], rims_ref.shape[1]
    lanes = lax.broadcasted_iota(jnp.int32, (count, groups * rim), 1).astype(F32) + float(grains)
    pick = jnp.where(lanes == column, 1.0, 0.0).astype(BF16)
    rims = rims_ref[...].reshape(groups * rim, rims_ref.shape[2])
    found = jnp.dot(pick, rims, preferred_element_type=F32)
    out[...] = (out[...].astype(F32) + found).astype(BF16)


def route_kernel(round_ref, place_ref, tables_ref, own_ref, rims_ref, send_ref, mine_ref):
    count = mine_ref.shape[0]
    columns = route_columns((round_ref[0] * count).astype(F32), place_ref[0], tables_ref, count)
    for column, out in zip(columns, [mine_ref] + [send_ref.at[j] for j in range(send_ref.shape[0])]):
        pick_own(column, own_ref, out)
        add_listed(column, rims_ref, own_ref.shape[2], out)


def exchange_kernel(n_ha, send_ref, recv_ref, relay_ref, send_sem, recv_sem):
    x, y, h = lax.axis_index("gx"), lax.axis_index("gy"), lax.axis_index("ha")
    right, left = (x, y, lax.rem(h + 1, n_ha)), (x, y, lax.rem(h + n_ha - 1, n_ha))
    half = send_ref.shape[1] // 2
    upper, lower = pl.ds(0, half), pl.ds(half, half)
    barrier = pltpu.get_barrier_semaphore()
    for device in (right, left):
        pl.semaphore_signal(barrier, inc=1, device_id=device, device_id_type=MESH)
    pl.semaphore_wait(barrier, 2)

    def send(source, landing, device, slot):
        copy = pltpu.make_async_remote_copy(
            src_ref=source,
            dst_ref=landing,
            send_sem=send_sem.at[slot],
            recv_sem=recv_sem.at[slot],
            device_id=device,
            device_id_type=MESH,
        )
        copy.start()
        return copy

    across = [
        send(send_ref.at[1, upper], relay_ref.at[0], right, 0),
        send(send_ref.at[1, lower], relay_ref.at[1], left, 1),
    ]
    direct = [
        send(send_ref.at[0], recv_ref.at[0], right, 2),
        send(send_ref.at[2], recv_ref.at[2], left, 3),
    ]
    across[0].wait_recv()
    onward = [send(relay_ref.at[0], recv_ref.at[1, upper], right, 4)]
    across[1].wait_recv()
    onward.append(send(relay_ref.at[1], recv_ref.at[1, lower], left, 5))
    for copy in across:
        copy.wait_send()
    for copy in direct + onward:
        copy.wait()


def apply_kernel(
    opening, round_ref, place_ref, tables_ref, mine_ref, recv_ref, upsample_ref, normal_ref, tangent_ref,
    before_ref, out_ref, pick_ref, rotated_ref,
):
    places = tables_ref.shape[0]
    count = mine_ref.shape[0]
    nodes, width = upsample_ref.shape
    lines = out_ref.shape[0] // (3 * width)
    grains = lines * 128
    step = padded(width)
    first = (round_ref[0] * count).astype(F32)
    place = place_ref[0]
    here = place.astype(F32)
    pick_ref[:count, :] = mine_ref[...]
    pick_ref[count:, :] = recv_ref[...]
    from_place, to_place = table_row(tables_ref, SOURCE_PLACE), table_row(tables_ref, TARGET_PLACE)
    every = jnp.concatenate([tables_ref[j] for j in range(places)], axis=1)
    picked_rows = []
    for j in range(places):
        there = lax.rem(place + places - j, places).astype(F32)
        picked_rows.append(chosen(from_place, to_place, there, here, first, count))
    select = jnp.concatenate(picked_rows, axis=0)
    table = lax.dot_general(select, every, NT, precision=lax.Precision.HIGHEST, preferred_element_type=F32)
    frame = [table[:, i : i + 1] for i in range(9)]

    def evaluate(begin, size):
        values = []
        for d in range(3):
            found = lax.dot_general(
                pick_ref[:, d * step : d * step + width],
                upsample_ref[pl.ds(begin, size), :],
                NT,
                preferred_element_type=F32,
            )
            values.append(found.astype(BF16).astype(F32))
        for c in range(3):
            turned = frame[3 * c] * values[0] + frame[3 * c + 1] * values[1] + frame[3 * c + 2] * values[2]
            rotated_ref[c, :, pl.ds(begin, size)] = turned.astype(BF16)

    tile = 256
    whole = nodes // tile

    def body(i, carry):
        evaluate(pl.multiple_of(i * tile, tile), tile)
        return carry

    lax.fori_loop(0, whole, body, 0)
    if nodes % tile:
        evaluate(whole * tile, nodes % tile)
    quad = [
        jnp.dot(rotated_ref[c], (normal_ref if c == 0 else tangent_ref)[...], preferred_element_type=F32)
        for c in range(3)
    ]
    scaling = table[:, SCALE : SCALE + 1]
    lanes = lax.broadcasted_iota(jnp.int32, (places * count, grains), 1).astype(F32)
    spot = jnp.where(lanes == table[:, TARGET_COLUMN : TARGET_COLUMN + 1], 1.0, 0.0).astype(BF16)
    for c in range(3):
        given = (frame[c] * quad[0] + frame[3 + c] * quad[1] + frame[6 + c] * quad[2]) * scaling
        high = given.astype(BF16)
        low = (given - high.astype(F32)).astype(BF16)
        total = lax.dot_general(high, spot, TN, preferred_element_type=F32)
        total += lax.dot_general(low, spot, TN, preferred_element_type=F32)
        for line in range(lines):
            spread = pl.ds(c * width * lines + line, width, stride=lines)
            part = slice(line * 128, (line + 1) * 128)
            before = before_ref[c, :, part] if opening else before_ref[spread, :]
            out_ref[spread, :] = total[:, part] + before


def shards(
    sizes,
    density,
    upsample,
    normal_kernel,
    tangent_kernel,
    self_operator,
    rim_list,
    pair_target,
    pair_source,
    pair_weight,
    pair_angles,
    live_count,
):
    places = sizes[2]
    width, grains = density.shape[1], density.shape[4]
    nodes = upsample.shape[0]
    rim = rim_list.shape[-1]
    slots = pair_source.shape[-1]
    span = 3 * padded(width)
    count = CAPACITY
    own = density.reshape(3, width, grains)
    normal, tangent = normal_kernel.T, tangent_kernel.T
    lines = grains // 128
    listed, table = pl.pallas_call(
        functools.partial(prepare_kernel, places),
        out_shape=[jax.ShapeDtypeStruct((rim, span), BF16), jax.ShapeDtypeStruct((TABLE, slots), F32)],
        in_specs=[SMEM] + [VMEM] * 6,
        out_specs=[VMEM, VMEM],
        compiler_params=limit(8),
        name="prepare",
    )(
        live_count.reshape(1),
        rim_list.reshape(1, rim),
        pair_target.reshape(1, slots),
        pair_source.reshape(1, slots),
        pair_weight.reshape(1, slots),
        pair_angles.reshape(3, 1, slots),
        own,
    )
    rims, tables, send, mine, most, base = pl.pallas_call(
        functools.partial(gather_kernel, sizes),
        out_shape=[
            jax.ShapeDtypeStruct((9, rim, span), BF16),
            jax.ShapeDtypeStruct((places, TABLE, slots), F32),
            jax.ShapeDtypeStruct((places - 1, count, span), BF16),
            jax.ShapeDtypeStruct((count, span), BF16),
            jax.ShapeDtypeStruct((1, 128), F32),
            jax.ShapeDtypeStruct((3, width, grains), F32),
        ],
        in_specs=[ANY, ANY, VMEM, VMEM],
        out_specs=[VMEM] * 6,
        scratch_shapes=[
            pltpu.SemaphoreType.DMA((places + 7,)),
            pltpu.SemaphoreType.DMA((places + 7,)),
            pltpu.SemaphoreType.DMA((2,)),
        ],
        compiler_params=limit(24, collective_id=0, has_side_effects=True),
        name="gather",
    )(listed, table, own, self_operator)
    place = lax.axis_index("ha").astype(jnp.int32).reshape(1)

    def route(turn):
        return pl.pallas_call(
            route_kernel,
            out_shape=[
                jax.ShapeDtypeStruct((places - 1, count, span), BF16),
                jax.ShapeDtypeStruct((count, span), BF16),
            ],
            in_specs=[SMEM, SMEM, VMEM, VMEM, VMEM],
            out_specs=[VMEM, VMEM],
            compiler_params=limit(24),
            name="route",
        )(turn, place, tables, own, rims)

    def exchange(send):
        return pl.pallas_call(
            functools.partial(exchange_kernel, places),
            out_shape=jax.ShapeDtypeStruct((places - 1, count, span), BF16),
            in_specs=[ANY],
            out_specs=ANY,
            scratch_shapes=[
                pltpu.VMEM((2, count // 2, span), BF16),
                pltpu.SemaphoreType.DMA((6,)),
                pltpu.SemaphoreType.DMA((6,)),
            ],
            compiler_params=limit(4, collective_id=1, has_side_effects=True),
            name="exchange",
        )(send).reshape((places - 1) * count, span)

    def apply(turn, mine, received, before, opening):
        return pl.pallas_call(
            functools.partial(apply_kernel, opening),
            out_shape=jax.ShapeDtypeStruct((3 * width * lines, 128), F32),
            in_specs=[SMEM, SMEM] + [VMEM] * 7,
            out_specs=VMEM,
            scratch_shapes=[
                pltpu.VMEM((places * count, span), BF16),
                pltpu.VMEM((3, places * count, nodes), BF16),
            ],
            compiler_params=limit(40),
            name="apply",
        )(turn, place, tables, mine, received, upsample, normal, tangent, before)

    turn = jnp.zeros((1,), jnp.int32)
    result = apply(turn, mine, exchange(send), base, True)
    rounds = (most[0, 0].astype(jnp.int32) + count - 1) // count

    def again(state):
        now, total = state
        send, mine = route(now.reshape(1))
        return now + 1, apply(now.reshape(1), mine, exchange(send), total, False)

    _, result = lax.while_loop(lambda state: state[0] < rounds, again, (jnp.int32(1), result))
    return result.reshape(3, width, 1, 1, grains)


def solution(mesh):
    sizes = tuple(mesh.shape[axis] for axis in ("gx", "gy", "ha"))
    return jax.shard_map(
        functools.partial(shards, sizes),
        mesh=mesh,
        in_specs=(
            P(None, None, "gx", "gy", "ha"),
            P(),
            P(),
            P(),
            P(),
            P("gx", "gy", "ha"),
            P("gx", "gy", "ha", None),
            P("gx", "gy", "ha", None),
            P("gx", "gy", "ha", None),
            P(None, "gx", "gy", "ha", None),
            P("gx", "gy", "ha"),
        ),
        out_specs=P(None, None, "gx", "gy", "ha"),
        check_vma=False,
    )
```

```python
import functools

import jax
import jax.numpy as jnp
from jax import lax
from jax.experimental import pallas as pl
from jax.experimental.pallas import tpu as pltpu
from jax.sharding import PartitionSpec as P

MESH = pl.DeviceIdType.MESH
ANY = pl.BlockSpec(memory_space=pl.ANY)
VMEM = pl.BlockSpec(memory_space=pltpu.VMEM)
SMEM = pl.BlockSpec(memory_space=pltpu.SMEM)
HBM = pl.BlockSpec(memory_space=pltpu.HBM)
CAPACITY = 96
TABLE = 16
SCALE, SOURCE_PLACE, SOURCE_COLUMN, TARGET_PLACE, TARGET_COLUMN = 9, 10, 11, 12, 13
NT = (((1,), (1,)), ((), ()))
TN = (((0,), (0,)), ((), ()))
F32 = jnp.float32
BF16 = jnp.bfloat16


def padded(width):
    return (width + 127) // 128 * 128


def limit(mebibytes, **others):
    return pltpu.CompilerParams(vmem_limit_bytes=mebibytes * 1024 * 1024, **others)


def split(value, size):
    bits = size.bit_length() - 1
    assert size == 1 << bits
    return lax.shift_right_logical(value, bits), value & (size - 1)


def load(sources, landings, sem):
    copies = [pltpu.make_async_copy(a, b, sem.at[i]) for i, (a, b) in enumerate(zip(sources, landings))]
    for copy in copies:
        copy.start()
    return copies


def prepare_kernel(
    places, live_ref, list_hbm, target_hbm, source_hbm, weight_hbm, angles_hbm, own_hbm, rim_ref, table_ref,
    list_ref, target_ref, source_ref, weight_ref, angles_ref, own_ref, sem,
):
    for copy in load(
        [list_hbm, target_hbm, source_hbm, weight_hbm, angles_hbm, own_hbm],
        [list_ref, target_ref, source_ref, weight_ref, angles_ref, own_ref],
        sem,
    ):
        copy.wait()
    width, grains = own_ref.shape[1:]
    rim, slots = list_ref.shape[1], source_ref.shape[1]
    step = padded(width)
    square = [lax.broadcasted_iota(jnp.int32, (rim, rim), axis) for axis in (0, 1)]
    listed = jnp.where(square[0] == square[1], list_ref[...].astype(F32), 0.0)
    listed = jnp.sum(listed, axis=1, keepdims=True)
    lanes = lax.broadcasted_iota(jnp.int32, (rim, grains), 1).astype(F32)
    pick = jnp.where(listed == lanes, 1.0, 0.0).astype(BF16)
    rim_ref[...] = jnp.zeros_like(rim_ref)
    for c in range(3):
        found = lax.dot_general(pick, own_ref[c], NT, preferred_element_type=F32)
        rim_ref[:, c * step : c * step + width] = found.astype(BF16)
    c0, c1, c2 = (jnp.cos(angles_ref[i]) for i in range(3))
    s0, s1, s2 = (jnp.sin(angles_ref[i]) for i in range(3))
    frame = [
        c0 * c1 * c2 - s0 * s2, -(c0 * c1 * s2) - s0 * c2, c0 * s1,
        s0 * c1 * c2 + c0 * s2, -(s0 * c1 * s2) + c0 * c2, s0 * s1,
        -(s1 * c2), s1 * s2, c1,
    ]
    alive = lax.broadcasted_iota(jnp.int32, (1, slots), 1) < live_ref[0]
    source = source_ref[...]
    inside = source < grains * places
    place, column = split(source, grains)
    group, within = split(jnp.maximum(source - grains * places, 0), rim * places)
    rim_place, rim_column = split(within, rim)
    target_place, target_column = split(target_ref[...], grains)
    rows = frame + [
        jnp.where(alive, weight_ref[...], 0.0),
        jnp.where(inside, place, rim_place).astype(F32),
        jnp.where(inside, column, grains + group * rim + rim_column).astype(F32),
        jnp.where(alive, target_place, -1).astype(F32),
        target_column.astype(F32),
    ]
    table_ref[...] = jnp.zeros_like(table_ref)
    for i, row in enumerate(rows):
        table_ref[i : i + 1, :] = row


def gather_kernel(
    sizes, rim_ref, table_ref, own_hbm, rims_ref, tables_ref, send_ref, mine_ref, most_ref, own_ref, send_sem, recv_sem, own_sem, load_sem,
):
    n_gx, n_gy, n_ha = sizes
    x, y, h = lax.axis_index("gx"), lax.axis_index("gy"), lax.axis_index("ha")
    loads = load([own_hbm], [own_ref], load_sem)
    near = 1 - 2 * lax.rem(y, 2)
    partner = (x, y + near, h)
    far = lax.rem(y - near + n_gy, n_gy)
    barrier = pltpu.get_barrier_semaphore()
    mates = [(x, y, lax.rem(h + j, n_ha)) for j in range(1, n_ha)]
    sides = [(lax.rem(x + dx + n_gx, n_gx), y, h) for dx in (-1, 1)]
    beyond = [(lax.rem(x + dx + n_gx, n_gx), far, h) for dx in (-1, 0, 1)]
    peers = mates + sides + beyond + [partner]
    for device in peers:
        pl.semaphore_signal(barrier, inc=1, device_id=device, device_id_type=MESH)
    own = [
        pltpu.make_async_copy(rim_ref, rims_ref.at[4], own_sem.at[0]),
        pltpu.make_async_copy(table_ref, tables_ref.at[h], own_sem.at[1]),
    ]
    for copy in own:
        copy.start()
    pl.semaphore_wait(barrier, len(peers))

    def send(source, landing, device, slot):
        copy = pltpu.make_async_remote_copy(
            src_ref=source,
            dst_ref=landing,
            send_sem=send_sem.at[slot],
            recv_sem=recv_sem.at[slot],
            device_id=device,
            device_id_type=MESH,
        )
        copy.start()
        return copy

    tables = [send(table_ref, tables_ref.at[h], mates[j], j) for j in range(n_ha - 1)]
    aside = [send(rim_ref, rims_ref.at[(1 - dx) * 3 + 1], sides[(dx + 1) // 2], n_ha + dx) for dx in (-1, 1)]
    rest = [
        send(rim_ref, rims_ref.at[(1 - dx) * 3 + 1 + near], beyond[dx + 1], n_ha + 3 + dx) for dx in (-1, 0, 1)
    ]
    rest.append(send(rim_ref, rims_ref.at[4 - near], partner, n_ha))
    for copy in loads:
        copy.wait()
    for copy in own:
        copy.wait()
    for copy in tables:
        copy.wait()
    columns = route_columns(jnp.float32(0.0), h, tables_ref, mine_ref.shape[0])
    outs = [mine_ref] + [send_ref.at[j] for j in range(n_ha - 1)]
    for column, out in zip(columns, outs):
        pick_own(column, own_ref, out)
    most_ref[...] = jnp.broadcast_to(longest(tables_ref), most_ref.shape)
    for i, dx in enumerate((-1, 1)):
        aside[i].wait_recv()
        rest.append(
            send(rims_ref.at[(1 - dx) * 3 + 1], rims_ref.at[(1 - dx) * 3 + 1 - near], partner, n_ha + 5 + i)
        )
    for copy in aside:
        copy.wait_send()
    for copy in rest:
        copy.wait()
    for column, out in zip(columns, outs):
        add_listed(column, rims_ref, own_ref.shape[2], out)


def ranks(mask):
    total, length = mask, mask.shape[1]
    lanes = lax.broadcasted_iota(jnp.int32, mask.shape, 1)
    step = 1
    while step < length:
        total = total + jnp.where(lanes >= step, pltpu.roll(total, step, 1), 0.0)
        step *= 2
    return total - mask


def table_row(tables_ref, row):
    return jnp.concatenate([tables_ref[j, row : row + 1, :] for j in range(tables_ref.shape[0])], axis=1)


def chosen(from_place, to_place, source, target, first, count):
    mask = jnp.where((from_place == source) & (to_place == target), 1.0, 0.0)
    key = jnp.where(mask > 0.0, ranks(mask) - first, -1.0)
    rows = lax.broadcasted_iota(jnp.int32, (count, mask.shape[1]), 0).astype(F32)
    return jnp.where(rows == key, 1.0, 0.0)


def route_columns(first, place, tables_ref, count):
    places = tables_ref.shape[0]
    here = place.astype(F32)
    from_place, to_place = table_row(tables_ref, SOURCE_PLACE), table_row(tables_ref, TARGET_PLACE)
    column_row = table_row(tables_ref, SOURCE_COLUMN) + 1.0
    columns = []
    for j in range(places):
        there = lax.rem(place + j, places).astype(F32)
        select = chosen(from_place, to_place, here, there, first, count)
        columns.append(jnp.sum(select * column_row, axis=1, keepdims=True) - 1.0)
    return columns


def longest(tables_ref):
    places = tables_ref.shape[0]
    from_place, to_place = table_row(tables_ref, SOURCE_PLACE), table_row(tables_ref, TARGET_PLACE)
    most = jnp.zeros((1, 1), F32)
    for source in range(places):
        for target in range(places):
            hit = jnp.where((from_place == float(source)) & (to_place == float(target)), 1.0, 0.0)
            most = jnp.maximum(most, jnp.sum(hit, axis=1, keepdims=True))
    return most


def pick_own(column, own_ref, out):
    count, (width, grains) = column.shape[0], own_ref.shape[1:]
    step = padded(width)
    lanes = lax.broadcasted_iota(jnp.int32, (count, grains), 1).astype(F32)
    pick = jnp.where(lanes == column, 1.0, 0.0).astype(BF16)
    out[...] = jnp.zeros(out.shape, BF16)
    for c in range(3):
        found = lax.dot_general(pick, own_ref[c], NT, preferred_element_type=F32)
        out[:, c * step : c * step + width] = found.astype(BF16)


def add_listed(column, rims_ref, grains, out):
    count, groups, rim = column.shape[0], rims_ref.shape[0], rims_ref.shape[1]
    lanes = lax.broadcasted_iota(jnp.int32, (count, groups * rim), 1).astype(F32) + float(grains)
    pick = jnp.where(lanes == column, 1.0, 0.0).astype(BF16)
    rims = rims_ref[...].reshape(groups * rim, rims_ref.shape[2])
    found = jnp.dot(pick, rims, preferred_element_type=F32)
    out[...] = (out[...].astype(F32) + found).astype(BF16)


def route_kernel(round_ref, place_ref, tables_ref, own_ref, rims_ref, send_ref, mine_ref):
    count = mine_ref.shape[0]
    columns = route_columns((round_ref[0] * count).astype(F32), place_ref[0], tables_ref, count)
    for column, out in zip(columns, [mine_ref] + [send_ref.at[j] for j in range(send_ref.shape[0])]):
        pick_own(column, own_ref, out)
        add_listed(column, rims_ref, own_ref.shape[2], out)


def finish_kernel(
    n_ha, opening, round_ref, tables_ref, mine_ref, send_ref, upsample_hbm, normal_hbm, tangent_hbm, *rest
):
    if opening:
        self_hbm, own_hbm, *rest = rest
    else:
        before_hbm, *rest = rest
    out_ref, recv_ref, relay_ref, upsample_ref, normal_ref, tangent_ref, table_ref, rotated_ref, sum_ref, *rest = rest
    if opening:
        self_ref, own_ref, *rest = rest
    else:
        before_ref, *rest = rest
    send_sem, recv_sem, load_sem = rest
    x, y, h = lax.axis_index("gx"), lax.axis_index("gy"), lax.axis_index("ha")
    right, left = (x, y, lax.rem(h + 1, n_ha)), (x, y, lax.rem(h + n_ha - 1, n_ha))
    count = mine_ref.shape[0]
    nodes, width = upsample_ref.shape
    grains = out_ref.shape[2]
    step = padded(width)
    half = count // 2
    upper, lower = pl.ds(0, half), pl.ds(half, half)
    loads = load(
        [upsample_hbm, normal_hbm, tangent_hbm] + ([self_hbm, own_hbm] if opening else [before_hbm]),
        [upsample_ref, normal_ref, tangent_ref] + ([self_ref, own_ref] if opening else [before_ref]),
        load_sem,
    )
    barrier = pltpu.get_barrier_semaphore()
    for device in (right, left):
        pl.semaphore_signal(barrier, inc=1, device_id=device, device_id_type=MESH)
    pl.semaphore_wait(barrier, 2)

    def send(source, landing, device, slot):
        copy = pltpu.make_async_remote_copy(
            src_ref=source,
            dst_ref=landing,
            send_sem=send_sem.at[slot],
            recv_sem=recv_sem.at[slot],
            device_id=device,
            device_id_type=MESH,
        )
        copy.start()
        return copy

    across = [
        send(send_ref.at[1, upper], relay_ref.at[0], right, 0),
        send(send_ref.at[1, lower], relay_ref.at[1], left, 1),
    ]
    direct = [
        send(send_ref.at[0], recv_ref.at[0], right, 2),
        send(send_ref.at[2], recv_ref.at[2], left, 3),
    ]

    first = (round_ref[0] * count).astype(F32)
    from_place, to_place = table_row(tables_ref, SOURCE_PLACE), table_row(tables_ref, TARGET_PLACE)
    every = jnp.concatenate([tables_ref[j] for j in range(n_ha)], axis=1)
    high = every.astype(BF16)
    middle = (every - high.astype(F32)).astype(BF16)
    low = (every - high.astype(F32) - middle.astype(F32)).astype(BF16)
    parts = jnp.concatenate([high, middle, low], axis=0)
    here = h.astype(F32)
    for j in range(n_ha):
        there = lax.rem(h + n_ha - j, n_ha).astype(F32)
        select = chosen(from_place, to_place, there, here, first, count).astype(BF16)
        found = lax.dot_general(select, parts, NT, preferred_element_type=F32)
        table_ref[j * count : (j + 1) * count, :] = (
            found[:, :TABLE] + found[:, TABLE : 2 * TABLE] + found[:, 2 * TABLE :]
        )

    def process(blocks, start, end):
        rows = len(blocks) * count
        table = jnp.concatenate([table_ref[j * count : (j + 1) * count, :] for j, _ in blocks], axis=0)
        frame = [table[:, i : i + 1] for i in range(9)]
        stacked = jnp.concatenate(
            [ref[:, d * step : d * step + width] for d in range(3) for _, ref in blocks], axis=0
        )

        def evaluate(begin, size):
            found = lax.dot_general(stacked, upsample_ref[pl.ds(begin, size), :], NT, preferred_element_type=F32)
            values = [found[d * rows : (d + 1) * rows].astype(BF16).astype(F32) for d in range(3)]
            for c in range(3):
                turned = frame[3 * c] * values[0] + frame[3 * c + 1] * values[1] + frame[3 * c + 2] * values[2]
                rotated_ref[c * rows : (c + 1) * rows, pl.ds(begin, size)] = turned.astype(BF16)

        tile = 256
        whole = nodes // tile

        def body(i, carry):
            evaluate(pl.multiple_of(i * tile, tile), tile)
            return carry

        lax.fori_loop(0, whole, body, 0)
        if nodes % tile:
            evaluate(whole * tile, nodes % tile)
        normal = jnp.dot(rotated_ref[:rows], normal_ref[...], preferred_element_type=F32)
        tangent = jnp.dot(rotated_ref[rows : 3 * rows], tangent_ref[...], preferred_element_type=F32)
        quad = [normal, tangent[:rows], tangent[rows:]]
        scaling = table[:, SCALE : SCALE + 1]
        lanes = lax.broadcasted_iota(jnp.int32, (rows, grains), 1).astype(F32)
        spot = jnp.where(lanes == table[:, TARGET_COLUMN : TARGET_COLUMN + 1], 1.0, 0.0).astype(BF16)
        spot = jnp.concatenate([spot, spot], axis=0)
        for c in range(3):
            given = (frame[c] * quad[0] + frame[3 + c] * quad[1] + frame[6 + c] * quad[2]) * scaling
            top = given.astype(BF16)
            rest = (given - top.astype(F32)).astype(BF16)
            total = lax.dot_general(jnp.concatenate([top, rest], axis=0), spot, TN, preferred_element_type=F32)
            if not start:
                total += sum_ref[c]
            if end:
                out_ref[c * width : (c + 1) * width, 0, :] = total
            else:
                sum_ref[c] = total

    for copy in loads:
        copy.wait()
    process([(0, mine_ref)], True, False)
    across[0].wait_recv()
    onward = [send(relay_ref.at[0], recv_ref.at[1, upper], right, 4)]
    across[1].wait_recv()
    onward.append(send(relay_ref.at[1], recv_ref.at[1, lower], left, 5))
    for copy in direct:
        copy.wait_recv()
    process([(1, recv_ref.at[0]), (3, recv_ref.at[2])], False, False)
    for c in range(3):
        if opening:
            sum_ref[c] += jnp.dot(self_ref[...], own_ref[c], preferred_element_type=F32)
        else:
            sum_ref[c] += before_ref[c * width : (c + 1) * width, 0, :]
    for copy in onward:
        copy.wait_recv()
    process([(2, recv_ref.at[1])], False, True)
    for copy in across + direct + onward:
        copy.wait_send()


def shards(
    sizes,
    density,
    upsample,
    normal_kernel,
    tangent_kernel,
    self_operator,
    rim_list,
    pair_target,
    pair_source,
    pair_weight,
    pair_angles,
    live_count,
):
    places = sizes[2]
    width, grains = density.shape[1], density.shape[4]
    nodes = upsample.shape[0]
    rim = rim_list.shape[-1]
    slots = pair_source.shape[-1]
    span = 3 * padded(width)
    count = CAPACITY
    own = density.reshape(3, width, grains)
    normal, tangent = normal_kernel.T, tangent_kernel.T
    listed, table = pl.pallas_call(
        functools.partial(prepare_kernel, places),
        out_shape=[jax.ShapeDtypeStruct((rim, span), BF16), jax.ShapeDtypeStruct((TABLE, slots), F32)],
        in_specs=[SMEM] + [HBM] * 6,
        out_specs=[VMEM, VMEM],
        scratch_shapes=[
            pltpu.VMEM((1, rim), jnp.int32),
            pltpu.VMEM((1, slots), jnp.int32),
            pltpu.VMEM((1, slots), jnp.int32),
            pltpu.VMEM((1, slots), F32),
            pltpu.VMEM((3, 1, slots), F32),
            pltpu.VMEM((3, width, grains), BF16),
            pltpu.SemaphoreType.DMA((6,)),
        ],
        compiler_params=limit(60),
        name="prepare",
    )(
        live_count.reshape(1),
        rim_list.reshape(1, rim),
        pair_target.reshape(1, slots),
        pair_source.reshape(1, slots),
        pair_weight.reshape(1, slots),
        pair_angles.reshape(3, 1, slots),
        own,
    )
    rims, tables, send, mine, most = pl.pallas_call(
        functools.partial(gather_kernel, sizes),
        out_shape=[
            jax.ShapeDtypeStruct((9, rim, span), BF16),
            jax.ShapeDtypeStruct((places, TABLE, slots), F32),
            jax.ShapeDtypeStruct((places - 1, count, span), BF16),
            jax.ShapeDtypeStruct((count, span), BF16),
            jax.ShapeDtypeStruct((1, 128), F32),
        ],
        in_specs=[ANY, ANY, HBM],
        out_specs=[VMEM] * 5,
        scratch_shapes=[
            pltpu.VMEM((3, width, grains), BF16),
            pltpu.SemaphoreType.DMA((places + 7,)),
            pltpu.SemaphoreType.DMA((places + 7,)),
            pltpu.SemaphoreType.DMA((2,)),
            pltpu.SemaphoreType.DMA((1,)),
        ],
        compiler_params=limit(24, collective_id=0, has_side_effects=True),
        name="gather",
    )(listed, table, own)
    place = lax.axis_index("ha").astype(jnp.int32).reshape(1)

    def route(turn):
        return pl.pallas_call(
            route_kernel,
            out_shape=[
                jax.ShapeDtypeStruct((places - 1, count, span), BF16),
                jax.ShapeDtypeStruct((count, span), BF16),
            ],
            in_specs=[SMEM, SMEM, VMEM, VMEM, VMEM],
            out_specs=[VMEM, VMEM],
            compiler_params=limit(24),
            name="route",
        )(turn, place, tables, own, rims)

    def finish(turn, mine, send, *last):
        opening = len(last) == 2
        shape = (3 * width, 1, grains)
        return pl.pallas_call(
            functools.partial(finish_kernel, places, opening),
            out_shape=jax.ShapeDtypeStruct(shape, F32),
            in_specs=[SMEM, VMEM, VMEM, ANY] + [HBM] * (3 + len(last)),
            out_specs=VMEM,
            scratch_shapes=[
                pltpu.VMEM((places - 1, count, span), BF16),
                pltpu.VMEM((2, count // 2, span), BF16),
                pltpu.VMEM((nodes, width), BF16),
                pltpu.VMEM((nodes, width), BF16),
                pltpu.VMEM((nodes, width), BF16),
                pltpu.VMEM((places * count, TABLE), F32),
                pltpu.VMEM((6 * count, nodes), BF16),
                pltpu.VMEM((3, width, grains), F32),
            ]
            + (
                [pltpu.VMEM((width, width), BF16), pltpu.VMEM((3, width, grains), BF16)]
                if opening
                else [pltpu.VMEM(shape, F32)]
            )
            + [
                pltpu.SemaphoreType.DMA((6,)),
                pltpu.SemaphoreType.DMA((6,)),
                pltpu.SemaphoreType.DMA((3 + len(last),)),
            ],
            compiler_params=limit(44, collective_id=1 if opening else 2, has_side_effects=True),
            name="finish",
        )(turn, tables, mine, send, upsample, normal, tangent, *last)

    turn = jnp.zeros((1,), jnp.int32)
    result = finish(turn, mine, send, self_operator, own)
    rounds = (most[0, 0].astype(jnp.int32) + count - 1) // count

    def again(state):
        now, total = state
        send, mine = route(now.reshape(1))
        return now + 1, finish(now.reshape(1), mine, send, total)

    _, result = lax.while_loop(lambda state: state[0] < rounds, again, (jnp.int32(1), result))
    return result.reshape(3, width, 1, 1, grains)


def solution(mesh):
    sizes = tuple(mesh.shape[axis] for axis in ("gx", "gy", "ha"))
    return jax.shard_map(
        functools.partial(shards, sizes),
        mesh=mesh,
        in_specs=(
            P(None, None, "gx", "gy", "ha"),
            P(),
            P(),
            P(),
            P(),
            P("gx", "gy", "ha"),
            P("gx", "gy", "ha", None),
            P("gx", "gy", "ha", None),
            P("gx", "gy", "ha", None),
            P(None, "gx", "gy", "ha", None),
            P("gx", "gy", "ha"),
        ),
        out_specs=P(None, None, "gx", "gy", "ha"),
        check_vma=False,
    )
```

```python
import functools

import jax
import jax.numpy as jnp
from jax import lax
from jax.experimental import pallas as pl
from jax.experimental.pallas import tpu as pltpu
from jax.sharding import PartitionSpec as P

MESH = pl.DeviceIdType.MESH
ANY = pl.BlockSpec(memory_space=pl.ANY)
VMEM = pl.BlockSpec(memory_space=pltpu.VMEM)
SMEM = pl.BlockSpec(memory_space=pltpu.SMEM)
HBM = pl.BlockSpec(memory_space=pltpu.HBM)
CAPACITY = 96
WIDE, NARROW = 1152, 256
TABLE = 16
SCALE, SOURCE_PLACE, SOURCE_COLUMN, TARGET_PLACE, TARGET_COLUMN = 9, 10, 11, 12, 13
NT = (((1,), (1,)), ((), ()))
TN = (((0,), (0,)), ((), ()))
F32 = jnp.float32
BF16 = jnp.bfloat16


def padded(width):
    return (width + 127) // 128 * 128


def limit(mebibytes, **others):
    return pltpu.CompilerParams(vmem_limit_bytes=mebibytes * 1024 * 1024, **others)


def split(value, size):
    bits = size.bit_length() - 1
    assert size == 1 << bits
    return lax.shift_right_logical(value, bits), value & (size - 1)


def load(sources, landings, sem):
    copies = [pltpu.make_async_copy(a, b, sem.at[i]) for i, (a, b) in enumerate(zip(sources, landings))]
    for copy in copies:
        copy.start()
    return copies


def prepare_kernel(
    places, live_ref, list_hbm, target_hbm, source_hbm, weight_hbm, angles_hbm, own_hbm, rim_ref, table_ref,
    list_ref, target_ref, source_ref, weight_ref, angles_ref, own_ref, sem,
):
    for copy in load(
        [list_hbm, target_hbm, source_hbm, weight_hbm, angles_hbm, own_hbm],
        [list_ref, target_ref, source_ref, weight_ref, angles_ref, own_ref],
        sem,
    ):
        copy.wait()
    width, grains = own_ref.shape[1:]
    rim, slots = list_ref.shape[1], source_ref.shape[1]
    step = padded(width)
    square = [lax.broadcasted_iota(jnp.int32, (rim, rim), axis) for axis in (0, 1)]
    listed = jnp.where(square[0] == square[1], list_ref[...].astype(F32), 0.0)
    listed = jnp.sum(listed, axis=1, keepdims=True)
    lanes = lax.broadcasted_iota(jnp.int32, (rim, grains), 1).astype(F32)
    pick = jnp.where(listed == lanes, 1.0, 0.0).astype(BF16)
    rim_ref[...] = jnp.zeros_like(rim_ref)
    for c in range(3):
        found = lax.dot_general(pick, own_ref[c], NT, preferred_element_type=F32)
        rim_ref[:, c * step : c * step + width] = found.astype(BF16)
    c0, c1, c2 = (jnp.cos(angles_ref[i]) for i in range(3))
    s0, s1, s2 = (jnp.sin(angles_ref[i]) for i in range(3))
    frame = [
        c0 * c1 * c2 - s0 * s2, -(c0 * c1 * s2) - s0 * c2, c0 * s1,
        s0 * c1 * c2 + c0 * s2, -(s0 * c1 * s2) + c0 * c2, s0 * s1,
        -(s1 * c2), s1 * s2, c1,
    ]
    alive = lax.broadcasted_iota(jnp.int32, (1, slots), 1) < live_ref[0]
    source = source_ref[...]
    inside = source < grains * places
    place, column = split(source, grains)
    group, within = split(jnp.maximum(source - grains * places, 0), rim * places)
    rim_place, rim_column = split(within, rim)
    target_place, target_column = split(target_ref[...], grains)
    rows = frame + [
        jnp.where(alive, weight_ref[...], 0.0),
        jnp.where(inside, place, rim_place).astype(F32),
        jnp.where(inside, column, grains + group * rim + rim_column).astype(F32),
        jnp.where(alive, target_place, -1).astype(F32),
        target_column.astype(F32),
    ]
    table_ref[...] = jnp.zeros_like(table_ref)
    for i, row in enumerate(rows):
        table_ref[i : i + 1, :] = row


def gather_kernel(
    sizes, rim_ref, table_ref, own_hbm, upsample_hbm, normal_hbm, tangent_hbm,
    rims_ref, tables_ref, send_ref, mine_ref, most_ref, upsample_ref, normal_ref, tangent_ref,
    own_ref, send_sem, recv_sem, own_sem, load_sem,
):
    n_gx, n_gy, n_ha = sizes
    x, y, h = lax.axis_index("gx"), lax.axis_index("gy"), lax.axis_index("ha")
    loads = load(
        [own_hbm, upsample_hbm, normal_hbm, tangent_hbm],
        [own_ref, upsample_ref, normal_ref, tangent_ref],
        load_sem,
    )
    near = 1 - 2 * lax.rem(y, 2)
    partner = (x, y + near, h)
    far = lax.rem(y - near + n_gy, n_gy)
    barrier = pltpu.get_barrier_semaphore()
    mates = [(x, y, lax.rem(h + j, n_ha)) for j in range(1, n_ha)]
    sides = [(lax.rem(x + dx + n_gx, n_gx), y, h) for dx in (-1, 1)]
    beyond = [(lax.rem(x + dx + n_gx, n_gx), far, h) for dx in (-1, 0, 1)]
    peers = mates + sides + beyond + [partner]
    for device in peers:
        pl.semaphore_signal(barrier, inc=1, device_id=device, device_id_type=MESH)
    own = [
        pltpu.make_async_copy(rim_ref, rims_ref.at[4], own_sem.at[0]),
        pltpu.make_async_copy(table_ref, tables_ref.at[h], own_sem.at[1]),
    ]
    for copy in own:
        copy.start()
    pl.semaphore_wait(barrier, len(peers))

    def send(source, landing, device, slot):
        copy = pltpu.make_async_remote_copy(
            src_ref=source,
            dst_ref=landing,
            send_sem=send_sem.at[slot],
            recv_sem=recv_sem.at[slot],
            device_id=device,
            device_id_type=MESH,
        )
        copy.start()
        return copy

    tables = [send(table_ref, tables_ref.at[h], mates[j], j) for j in range(n_ha - 1)]
    aside = [send(rim_ref, rims_ref.at[(1 - dx) * 3 + 1], sides[(dx + 1) // 2], n_ha + dx) for dx in (-1, 1)]
    rest = [
        send(rim_ref, rims_ref.at[(1 - dx) * 3 + 1 + near], beyond[dx + 1], n_ha + 3 + dx) for dx in (-1, 0, 1)
    ]
    rest.append(send(rim_ref, rims_ref.at[4 - near], partner, n_ha))
    loads[0].wait()
    for copy in own:
        copy.wait()
    for copy in tables:
        copy.wait()
    columns = route_columns(jnp.float32(0.0), h, tables_ref, mine_ref.shape[0])
    outs = [mine_ref] + [send_ref.at[j] for j in range(n_ha - 1)]
    for column, out in zip(columns, outs):
        pick_own(column, own_ref, out)
    most_ref[...] = jnp.broadcast_to(longest(tables_ref), most_ref.shape)
    for i, dx in enumerate((-1, 1)):
        aside[i].wait_recv()
        rest.append(
            send(rims_ref.at[(1 - dx) * 3 + 1], rims_ref.at[(1 - dx) * 3 + 1 - near], partner, n_ha + 5 + i)
        )
    for copy in aside:
        copy.wait_send()
    for copy in loads[1:]:
        copy.wait()
    for copy in rest:
        copy.wait()
    for column, out in zip(columns, outs):
        add_listed(column, rims_ref, own_ref.shape[2], out)


def ranks(mask):
    total, length = mask, mask.shape[1]
    lanes = lax.broadcasted_iota(jnp.int32, mask.shape, 1)
    step = 1
    while step < length:
        total = total + jnp.where(lanes >= step, pltpu.roll(total, step, 1), 0.0)
        step *= 2
    return total - mask


def table_row(tables_ref, row):
    return jnp.concatenate([tables_ref[j, row : row + 1, :] for j in range(tables_ref.shape[0])], axis=1)


def chosen(from_place, to_place, source, target, first, count):
    mask = jnp.where((from_place == source) & (to_place == target), 1.0, 0.0)
    key = jnp.where(mask > 0.0, ranks(mask) - first, -1.0)
    rows = lax.broadcasted_iota(jnp.int32, (count, mask.shape[1]), 0).astype(F32)
    return jnp.where(rows == key, 1.0, 0.0)


def route_columns(first, place, tables_ref, count):
    places = tables_ref.shape[0]
    here = place.astype(F32)
    from_place, to_place = table_row(tables_ref, SOURCE_PLACE), table_row(tables_ref, TARGET_PLACE)
    column_row = table_row(tables_ref, SOURCE_COLUMN) + 1.0
    columns = []
    for j in range(places):
        there = lax.rem(place + j, places).astype(F32)
        select = chosen(from_place, to_place, here, there, first, count)
        columns.append(jnp.sum(select * column_row, axis=1, keepdims=True) - 1.0)
    return columns


def longest(tables_ref):
    places = tables_ref.shape[0]
    from_place, to_place = table_row(tables_ref, SOURCE_PLACE), table_row(tables_ref, TARGET_PLACE)
    most = jnp.zeros((1, 1), F32)
    for source in range(places):
        for target in range(places):
            hit = jnp.where((from_place == float(source)) & (to_place == float(target)), 1.0, 0.0)
            most = jnp.maximum(most, jnp.sum(hit, axis=1, keepdims=True))
    return most


def pick_own(column, own_ref, out):
    count, (width, grains) = column.shape[0], own_ref.shape[1:]
    step = padded(width)
    lanes = lax.broadcasted_iota(jnp.int32, (count, grains), 1).astype(F32)
    pick = jnp.where(lanes == column, 1.0, 0.0).astype(BF16)
    out[...] = jnp.zeros(out.shape, BF16)
    for c in range(3):
        found = lax.dot_general(pick, own_ref[c], NT, preferred_element_type=F32)
        out[:, c * step : c * step + width] = found.astype(BF16)


def add_listed(column, rims_ref, grains, out):
    count, groups, rim = column.shape[0], rims_ref.shape[0], rims_ref.shape[1]
    lanes = lax.broadcasted_iota(jnp.int32, (count, groups * rim), 1).astype(F32) + float(grains)
    pick = jnp.where(lanes == column, 1.0, 0.0).astype(BF16)
    rims = rims_ref[...].reshape(groups * rim, rims_ref.shape[2])
    found = jnp.dot(pick, rims, preferred_element_type=F32)
    out[...] = (out[...].astype(F32) + found).astype(BF16)


def route_kernel(round_ref, place_ref, tables_ref, own_ref, rims_ref, send_ref, mine_ref):
    count = mine_ref.shape[0]
    columns = route_columns((round_ref[0] * count).astype(F32), place_ref[0], tables_ref, count)
    for column, out in zip(columns, [mine_ref] + [send_ref.at[j] for j in range(send_ref.shape[0])]):
        pick_own(column, own_ref, out)
        add_listed(column, rims_ref, own_ref.shape[2], out)


def add_pairs(table, blocks, upsample_ref, normal_ref, tangent_ref, rotated_ref, grains, tile, pause=None):
    nodes, width = upsample_ref.shape
    rows = table.shape[0]
    step = padded(width)
    frame = [table[:, i : i + 1] for i in range(9)]
    stacked = jnp.concatenate([ref[:, d * step : d * step + width] for d in range(3) for ref in blocks], axis=0)

    def evaluate(begin, size):
        found = lax.dot_general(stacked, upsample_ref[pl.ds(begin, size), :], NT, preferred_element_type=F32)
        values = [found[d * rows : (d + 1) * rows].astype(BF16).astype(F32) for d in range(3)]
        for c in range(3):
            turned = frame[3 * c] * values[0] + frame[3 * c + 1] * values[1] + frame[3 * c + 2] * values[2]
            rotated_ref[c * rows : (c + 1) * rows, pl.ds(begin, size)] = turned.astype(BF16)

    if tile >= 1024:
        for begin in range(0, nodes, tile):
            evaluate(begin, min(tile, nodes - begin))
    else:

        def body(i, carry):
            evaluate(pl.multiple_of(i * tile, tile), tile)
            return carry

        lax.fori_loop(0, nodes // tile, body, 0)
        if nodes % tile:
            evaluate(nodes // tile * tile, nodes % tile)
    if pause is not None:
        pause()
    normal = jnp.dot(rotated_ref[:rows], normal_ref[...], preferred_element_type=F32)
    tangent = jnp.dot(rotated_ref[rows : 3 * rows], tangent_ref[...], preferred_element_type=F32)
    quad = [normal, tangent[:rows], tangent[rows:]]
    scaling = table[:, SCALE : SCALE + 1]
    lanes = lax.broadcasted_iota(jnp.int32, (rows, grains), 1).astype(F32)
    spot = jnp.where(lanes == table[:, TARGET_COLUMN : TARGET_COLUMN + 1], 1.0, 0.0).astype(BF16)
    spot = jnp.concatenate([spot, spot], axis=0)
    totals = []
    for c in range(3):
        given = (frame[c] * quad[0] + frame[3 + c] * quad[1] + frame[6 + c] * quad[2]) * scaling
        top = given.astype(BF16)
        rest = (given - top.astype(F32)).astype(BF16)
        totals.append(
            lax.dot_general(jnp.concatenate([top, rest], axis=0), spot, TN, preferred_element_type=F32)
        )
    return totals


def exchange_kernel(
    n_ha, opening, tile, round_ref, tables_ref, mine_ref, send_ref, upsample_ref, normal_ref, tangent_ref, *rest
):
    if opening:
        self_ref, own_ref, *rest = rest
    sum_ref, last_ref, table_ref, near_ref, relay_ref, all_ref, rotated_ref, send_sem, recv_sem = rest
    x, y, h = lax.axis_index("gx"), lax.axis_index("gy"), lax.axis_index("ha")
    right, left = (x, y, lax.rem(h + 1, n_ha)), (x, y, lax.rem(h + n_ha - 1, n_ha))
    count = mine_ref.shape[0]
    grains = sum_ref.shape[2]
    half = count // 2
    upper, lower = pl.ds(0, half), pl.ds(half, half)
    barrier = pltpu.get_barrier_semaphore()
    for device in (right, left):
        pl.semaphore_signal(barrier, inc=1, device_id=device, device_id_type=MESH)
    pl.semaphore_wait(barrier, 2)

    def send(source, landing, device, slot):
        copy = pltpu.make_async_remote_copy(
            src_ref=source,
            dst_ref=landing,
            send_sem=send_sem.at[slot],
            recv_sem=recv_sem.at[slot],
            device_id=device,
            device_id_type=MESH,
        )
        copy.start()
        return copy

    direct = [
        send(send_ref.at[0], near_ref.at[0], right, 2),
        send(send_ref.at[2], near_ref.at[1], left, 3),
    ]

    first = (round_ref[0] * count).astype(F32)
    from_place, to_place = table_row(tables_ref, SOURCE_PLACE), table_row(tables_ref, TARGET_PLACE)
    every = jnp.concatenate([tables_ref[j] for j in range(n_ha)], axis=1)
    high = every.astype(BF16)
    middle = (every - high.astype(F32)).astype(BF16)
    low = (every - high.astype(F32) - middle.astype(F32)).astype(BF16)
    parts = jnp.concatenate([high, middle, low], axis=0)
    here = h.astype(F32)
    for place, j in enumerate((0, 1, 3, 2)):
        there = lax.rem(h + n_ha - j, n_ha).astype(F32)
        select = chosen(from_place, to_place, there, here, first, count).astype(BF16)
        found = lax.dot_general(select, parts, NT, preferred_element_type=F32)
        found = found[:, :TABLE] + found[:, TABLE : 2 * TABLE] + found[:, 2 * TABLE :]
        if j == 2:
            table_ref[...] = found
        else:
            all_ref[place * count : (place + 1) * count, :] = found
    weights = (upsample_ref, normal_ref, tangent_ref, rotated_ref, grains, tile)
    totals = add_pairs(all_ref[:count, :], [mine_ref], *weights)
    for c in range(3):
        total = totals[c]
        if opening:
            total += jnp.dot(self_ref[...], own_ref[c], preferred_element_type=F32)
        sum_ref[c] = total
    for copy in direct:
        copy.wait_send()
    across = [
        send(send_ref.at[1, upper], relay_ref.at[0], right, 0),
        send(send_ref.at[1, lower], relay_ref.at[1], left, 1),
    ]
    for copy in direct:
        copy.wait_recv()
    onward = []

    def pause():
        across[0].wait_recv()
        onward.append(send(relay_ref.at[0], last_ref.at[upper], right, 4))
        across[1].wait_recv()
        onward.append(send(relay_ref.at[1], last_ref.at[lower], left, 5))

    totals = add_pairs(all_ref[count:, :], [near_ref.at[0], near_ref.at[1]], *weights, pause)
    for c in range(3):
        sum_ref[c] += totals[c]
    for copy in across:
        copy.wait_send()
    for copy in onward:
        copy.wait()


def close_kernel(tile, sum_ref, last_ref, table_ref, upsample_ref, normal_ref, tangent_ref, *rest):
    *before, out_ref, rotated_ref = rest
    width, grains = sum_ref.shape[1:]
    totals = add_pairs(
        table_ref[...], [last_ref], upsample_ref, normal_ref, tangent_ref, rotated_ref, grains, tile
    )
    for c in range(3):
        total = totals[c] + sum_ref[c]
        if before:
            total += before[0][c * width : (c + 1) * width, 0, :]
        out_ref[c * width : (c + 1) * width, 0, :] = total


def shards(
    sizes,
    density,
    upsample,
    normal_kernel,
    tangent_kernel,
    self_operator,
    rim_list,
    pair_target,
    pair_source,
    pair_weight,
    pair_angles,
    live_count,
):
    places = sizes[2]
    width, grains = density.shape[1], density.shape[4]
    nodes = upsample.shape[0]
    rim = rim_list.shape[-1]
    slots = pair_source.shape[-1]
    span = 3 * padded(width)
    count = CAPACITY
    own = density.reshape(3, width, grains)
    normal, tangent = normal_kernel.T, tangent_kernel.T
    listed, table = pl.pallas_call(
        functools.partial(prepare_kernel, places),
        out_shape=[jax.ShapeDtypeStruct((rim, span), BF16), jax.ShapeDtypeStruct((TABLE, slots), F32)],
        in_specs=[SMEM] + [HBM] * 6,
        out_specs=[VMEM, VMEM],
        scratch_shapes=[
            pltpu.VMEM((1, rim), jnp.int32),
            pltpu.VMEM((1, slots), jnp.int32),
            pltpu.VMEM((1, slots), jnp.int32),
            pltpu.VMEM((1, slots), F32),
            pltpu.VMEM((3, 1, slots), F32),
            pltpu.VMEM((3, width, grains), BF16),
            pltpu.SemaphoreType.DMA((6,)),
        ],
        compiler_params=limit(60),
        name="prepare",
    )(
        live_count.reshape(1),
        rim_list.reshape(1, rim),
        pair_target.reshape(1, slots),
        pair_source.reshape(1, slots),
        pair_weight.reshape(1, slots),
        pair_angles.reshape(3, 1, slots),
        own,
    )
    rims, tables, send, mine, most, *weights = pl.pallas_call(
        functools.partial(gather_kernel, sizes),
        out_shape=[
            jax.ShapeDtypeStruct((9, rim, span), BF16),
            jax.ShapeDtypeStruct((places, TABLE, slots), F32),
            jax.ShapeDtypeStruct((places - 1, count, span), BF16),
            jax.ShapeDtypeStruct((count, span), BF16),
            jax.ShapeDtypeStruct((1, 128), F32),
            jax.ShapeDtypeStruct((nodes, width), BF16),
            jax.ShapeDtypeStruct((nodes, width), BF16),
            jax.ShapeDtypeStruct((nodes, width), BF16),
        ],
        in_specs=[ANY, ANY] + [HBM] * 4,
        out_specs=[VMEM] * 8,
        scratch_shapes=[
            pltpu.VMEM((3, width, grains), BF16),
            pltpu.SemaphoreType.DMA((places + 7,)),
            pltpu.SemaphoreType.DMA((places + 7,)),
            pltpu.SemaphoreType.DMA((2,)),
            pltpu.SemaphoreType.DMA((4,)),
        ],
        compiler_params=limit(24, collective_id=0, has_side_effects=True),
        name="gather",
    )(listed, table, own, upsample, normal, tangent)
    place = lax.axis_index("ha").astype(jnp.int32).reshape(1)

    def route(turn):
        return pl.pallas_call(
            route_kernel,
            out_shape=[
                jax.ShapeDtypeStruct((places - 1, count, span), BF16),
                jax.ShapeDtypeStruct((count, span), BF16),
            ],
            in_specs=[SMEM, SMEM, VMEM, VMEM, VMEM],
            out_specs=[VMEM, VMEM],
            compiler_params=limit(24),
            name="route",
        )(turn, place, tables, own, rims)

    def finish(turn, mine, send, before):
        opening = before is None
        tile = WIDE if opening else NARROW
        held = weights if opening else [upsample, normal, tangent]
        mixed = [self_operator, own] if opening else []
        total, last, rows = pl.pallas_call(
            functools.partial(exchange_kernel, places, opening, tile),
            out_shape=[
                jax.ShapeDtypeStruct((3, width, grains), F32),
                jax.ShapeDtypeStruct((count, span), BF16),
                jax.ShapeDtypeStruct((count, TABLE), F32),
            ],
            in_specs=[SMEM, VMEM, VMEM, ANY] + [VMEM] * (3 + len(mixed)),
            out_specs=[VMEM] * 3,
            scratch_shapes=[
                pltpu.VMEM((2, count, span), BF16),
                pltpu.VMEM((2, count // 2, span), BF16),
                pltpu.VMEM((3 * count, TABLE), F32),
                pltpu.VMEM((6 * count, nodes), BF16),
                pltpu.SemaphoreType.DMA((6,)),
                pltpu.SemaphoreType.DMA((6,)),
            ],
            compiler_params=limit(30, collective_id=1 if opening else 2, has_side_effects=True),
            name="exchange",
        )(turn, tables, mine, send, *held, *mixed)
        ended = [] if opening else [before]
        return pl.pallas_call(
            functools.partial(close_kernel, tile),
            out_shape=jax.ShapeDtypeStruct((3 * width, 1, grains), F32),
            in_specs=[VMEM] * (6 + len(ended)),
            out_specs=VMEM,
            scratch_shapes=[pltpu.VMEM((3 * count, nodes), BF16)],
            compiler_params=limit(30),
            name="close",
        )(total, last, rows, *held, *ended)

    turn = jnp.zeros((1,), jnp.int32)
    result = finish(turn, mine, send, None)
    result, most = lax.optimization_barrier((result, most))
    rounds = (most[0, 0].astype(jnp.int32) + count - 1) // count

    def again(state):
        now, total = state
        send, mine = route(now.reshape(1))
        return now + 1, finish(now.reshape(1), mine, send, total)

    _, result = lax.while_loop(lambda state: state[0] < rounds, again, (jnp.int32(1), result))
    return result.reshape(3, width, 1, 1, grains)


def solution(mesh):
    sizes = tuple(mesh.shape[axis] for axis in ("gx", "gy", "ha"))
    return jax.shard_map(
        functools.partial(shards, sizes),
        mesh=mesh,
        in_specs=(
            P(None, None, "gx", "gy", "ha"),
            P(),
            P(),
            P(),
            P(),
            P("gx", "gy", "ha"),
            P("gx", "gy", "ha", None),
            P("gx", "gy", "ha", None),
            P("gx", "gy", "ha", None),
            P(None, "gx", "gy", "ha", None),
            P("gx", "gy", "ha"),
        ),
        out_specs=P(None, None, "gx", "gy", "ha"),
        check_vma=False,
    )
```

```python
import functools

import jax
import jax.numpy as jnp
from jax import lax
from jax.experimental import pallas as pl
from jax.experimental.pallas import tpu as pltpu
from jax.sharding import PartitionSpec as P

MESH = pl.DeviceIdType.MESH
ANY = pl.BlockSpec(memory_space=pl.ANY)
VMEM = pl.BlockSpec(memory_space=pltpu.VMEM)
SMEM = pl.BlockSpec(memory_space=pltpu.SMEM)
HBM = pl.BlockSpec(memory_space=pltpu.HBM)
CAPACITY = 88
WIDE, NARROW = 1152, 256
TABLE = 16
SCALE, SOURCE_PLACE, SOURCE_COLUMN, TARGET_PLACE, TARGET_COLUMN = 9, 10, 11, 12, 13
NT = (((1,), (1,)), ((), ()))
TN = (((0,), (0,)), ((), ()))
F32 = jnp.float32
BF16 = jnp.bfloat16


def padded(width):
    return (width + 127) // 128 * 128


def limit(mebibytes, **others):
    return pltpu.CompilerParams(vmem_limit_bytes=mebibytes * 1024 * 1024, **others)


def split(value, size):
    bits = size.bit_length() - 1
    assert size == 1 << bits
    return lax.shift_right_logical(value, bits), value & (size - 1)


def load(sources, landings, sem):
    copies = [pltpu.make_async_copy(a, b, sem.at[i]) for i, (a, b) in enumerate(zip(sources, landings))]
    for copy in copies:
        copy.start()
    return copies


def prepare_kernel(
    places, live_ref, list_hbm, target_hbm, source_hbm, weight_hbm, angles_hbm, own_hbm, rim_ref, table_ref,
    list_ref, target_ref, source_ref, weight_ref, angles_ref, own_ref, sem,
):
    for copy in load(
        [list_hbm, target_hbm, source_hbm, weight_hbm, angles_hbm, own_hbm],
        [list_ref, target_ref, source_ref, weight_ref, angles_ref, own_ref],
        sem,
    ):
        copy.wait()
    width, grains = own_ref.shape[1:]
    rim, slots = list_ref.shape[1], source_ref.shape[1]
    step = padded(width)
    square = [lax.broadcasted_iota(jnp.int32, (rim, rim), axis) for axis in (0, 1)]
    listed = jnp.where(square[0] == square[1], list_ref[...].astype(F32), 0.0)
    listed = jnp.sum(listed, axis=1, keepdims=True)
    lanes = lax.broadcasted_iota(jnp.int32, (rim, grains), 1).astype(F32)
    pick = jnp.where(listed == lanes, 1.0, 0.0).astype(BF16)
    rim_ref[...] = jnp.zeros_like(rim_ref)
    for c in range(3):
        found = lax.dot_general(pick, own_ref[c], NT, preferred_element_type=F32)
        rim_ref[:, c * step : c * step + width] = found.astype(BF16)
    c0, c1, c2 = (jnp.cos(angles_ref[i]) for i in range(3))
    s0, s1, s2 = (jnp.sin(angles_ref[i]) for i in range(3))
    frame = [
        c0 * c1 * c2 - s0 * s2, -(c0 * c1 * s2) - s0 * c2, c0 * s1,
        s0 * c1 * c2 + c0 * s2, -(s0 * c1 * s2) + c0 * c2, s0 * s1,
        -(s1 * c2), s1 * s2, c1,
    ]
    alive = lax.broadcasted_iota(jnp.int32, (1, slots), 1) < live_ref[0]
    source = source_ref[...]
    inside = source < grains * places
    place, column = split(source, grains)
    group, within = split(jnp.maximum(source - grains * places, 0), rim * places)
    rim_place, rim_column = split(within, rim)
    target_place, target_column = split(target_ref[...], grains)
    rows = frame + [
        jnp.where(alive, weight_ref[...], 0.0),
        jnp.where(inside, place, rim_place).astype(F32),
        jnp.where(inside, column, grains + group * rim + rim_column).astype(F32),
        jnp.where(alive, target_place, -1).astype(F32),
        target_column.astype(F32),
    ]
    table_ref[...] = jnp.zeros_like(table_ref)
    for i, row in enumerate(rows):
        table_ref[i : i + 1, :] = row


def gather_kernel(
    sizes, rim_ref, table_ref, own_hbm, upsample_hbm, normal_hbm, tangent_hbm,
    rims_ref, tables_ref, send_ref, mine_ref, most_ref, upsample_ref, normal_ref, tangent_ref,
    own_ref, send_sem, recv_sem, own_sem, load_sem,
):
    n_gx, n_gy, n_ha = sizes
    x, y, h = lax.axis_index("gx"), lax.axis_index("gy"), lax.axis_index("ha")
    loads = load(
        [own_hbm, upsample_hbm, normal_hbm, tangent_hbm],
        [own_ref, upsample_ref, normal_ref, tangent_ref],
        load_sem,
    )
    near = 1 - 2 * lax.rem(y, 2)
    partner = (x, y + near, h)
    far = lax.rem(y - near + n_gy, n_gy)
    barrier = pltpu.get_barrier_semaphore()
    mates = [(x, y, lax.rem(h + j, n_ha)) for j in range(1, n_ha)]
    sides = [(lax.rem(x + dx + n_gx, n_gx), y, h) for dx in (-1, 1)]
    beyond = [(lax.rem(x + dx + n_gx, n_gx), far, h) for dx in (-1, 1)]
    ahead = (x, far, h)
    relays = lax.rem(x, 2) == lax.rem(y, 2)
    peers = mates + sides + beyond + [ahead, partner]
    for device in peers:
        pl.semaphore_signal(barrier, inc=1, device_id=device, device_id_type=MESH)
    own = [
        pltpu.make_async_copy(rim_ref, rims_ref.at[4], own_sem.at[0]),
        pltpu.make_async_copy(table_ref, tables_ref.at[h], own_sem.at[1]),
    ]
    for copy in own:
        copy.start()
    pl.semaphore_wait(barrier, len(peers))

    def send(source, landing, device, leaving, arriving):
        return pltpu.make_async_remote_copy(
            src_ref=source,
            dst_ref=landing,
            send_sem=send_sem.at[leaving],
            recv_sem=recv_sem.at[arriving],
            device_id=device,
            device_id_type=MESH,
        )

    tables = [send(table_ref, tables_ref.at[h], mates[j], j, j) for j in range(n_ha - 1)]
    for copy in tables:
        copy.start()
    aside, middle, onward, wide, across = [], [], [], [], []
    for i, dx in enumerate((-1, 1)):
        column, away = (dx + 1) * 3 + 1, (1 - dx) * 3 + 1
        aside.append(send(rim_ref, rims_ref.at[away], sides[i], n_ha + i, n_ha + 1 - i))
        onward.append(send(rims_ref.at[column], rims_ref.at[column - near], partner, n_ha + 2 + i, n_ha + 2 + i))
        across.append(send(rims_ref.at[column], rims_ref.at[column + near], ahead, n_ha + 4 + i, n_ha + 8 + i))
        wide.append(send(rim_ref, rims_ref.at[away + near], beyond[i], n_ha + 6 + i, n_ha + 9 - i))
    middle = [
        send(rim_ref, rims_ref.at[4 - near], partner, n_ha + 8, n_ha + 4),
        send(rim_ref, rims_ref.at[4 + near], ahead, n_ha + 9, n_ha + 5),
    ]
    for copy in aside + middle:
        copy.start()

    @pl.when(relays)
    def _():
        for copy in wide:
            copy.start()

    loads[0].wait()
    for copy in own:
        copy.wait()
    for copy in tables:
        copy.wait()
    column = route_columns(jnp.float32(0.0), h, tables_ref, mine_ref.shape[0])
    outs = [mine_ref] + [send_ref.at[j] for j in range(n_ha - 1)]
    pick_own(column, own_ref, outs)
    most_ref[...] = jnp.broadcast_to(longest(tables_ref), most_ref.shape)
    for copy in aside:
        copy.wait_recv()
    for copy in onward:
        copy.start()

    @pl.when(relays)
    def _():
        for copy in across:
            copy.start()

    for copy in loads[1:]:
        copy.wait()
    for copy in aside:
        copy.wait_send()
    for copy in middle + onward:
        copy.wait()
    for copy in across:
        copy.wait_recv()

    @pl.when(relays)
    def _():
        for copy in wide + across:
            copy.wait_send()

    add_listed(column, rims_ref, own_ref.shape[2], outs)


def ranks(mask):
    total, length = mask, mask.shape[1]
    lanes = lax.broadcasted_iota(jnp.int32, mask.shape, 1)
    step = 1
    while step < length:
        total = total + jnp.where(lanes >= step, pltpu.roll(total, step, 1), 0.0)
        step *= 2
    return total - mask


def table_row(tables_ref, row):
    return jnp.concatenate([tables_ref[j, row : row + 1, :] for j in range(tables_ref.shape[0])], axis=1)


def chosen(from_place, to_place, source, target, first, count):
    mask = jnp.where((from_place == source) & (to_place == target), 1.0, 0.0)
    key = jnp.where(mask > 0.0, ranks(mask) - first, -1.0)
    rows = lax.broadcasted_iota(jnp.int32, (count, mask.shape[1]), 0).astype(F32)
    return jnp.where(rows == key, 1.0, 0.0)


def route_columns(first, place, tables_ref, count):
    places = tables_ref.shape[0]
    here = place.astype(F32)
    from_place, to_place = table_row(tables_ref, SOURCE_PLACE), table_row(tables_ref, TARGET_PLACE)
    column_row = table_row(tables_ref, SOURCE_COLUMN) + 1.0
    columns = []
    for j in range(places):
        there = lax.rem(place + j, places).astype(F32)
        select = chosen(from_place, to_place, here, there, first, count)
        columns.append(jnp.sum(select * column_row, axis=1, keepdims=True) - 1.0)
    return jnp.concatenate(columns, axis=0)


def longest(tables_ref):
    places = tables_ref.shape[0]
    from_place, to_place = table_row(tables_ref, SOURCE_PLACE), table_row(tables_ref, TARGET_PLACE)
    most = jnp.zeros((1, 1), F32)
    for source in range(places):
        for target in range(places):
            hit = jnp.where((from_place == float(source)) & (to_place == float(target)), 1.0, 0.0)
            most = jnp.maximum(most, jnp.sum(hit, axis=1, keepdims=True))
    return most


def pick_own(column, own_ref, outs):
    rows, (width, grains) = column.shape[0], own_ref.shape[1:]
    step, count = padded(width), outs[0].shape[0]
    lanes = lax.broadcasted_iota(jnp.int32, (rows, grains), 1).astype(F32)
    pick = jnp.where(lanes == column, 1.0, 0.0).astype(BF16)
    for out in outs:
        out[...] = jnp.zeros(out.shape, BF16)
    for c in range(3):
        found = lax.dot_general(pick, own_ref[c], NT, preferred_element_type=F32)
        for j, out in enumerate(outs):
            out[:, c * step : c * step + width] = found[j * count : (j + 1) * count].astype(BF16)


def add_listed(column, rims_ref, grains, outs):
    rows, groups, rim = column.shape[0], rims_ref.shape[0], rims_ref.shape[1]
    span, count = rims_ref.shape[2], outs[0].shape[0]
    lanes = lax.broadcasted_iota(jnp.int32, (rows, groups * rim), 1).astype(F32) + float(grains)
    pick = jnp.where(lanes == column, 1.0, 0.0).astype(BF16)
    for begin in range(0, span, span // 3):
        part = slice(begin, begin + span // 3)
        rims = rims_ref[:, :, part].reshape(groups * rim, span // 3)
        found = jnp.dot(pick, rims, preferred_element_type=F32)
        for j, out in enumerate(outs):
            out[:, part] = (out[:, part].astype(F32) + found[j * count : (j + 1) * count]).astype(BF16)


def route_kernel(round_ref, place_ref, tables_ref, own_ref, rims_ref, send_ref, mine_ref):
    count = mine_ref.shape[0]
    column = route_columns((round_ref[0] * count).astype(F32), place_ref[0], tables_ref, count)
    outs = [mine_ref] + [send_ref.at[j] for j in range(send_ref.shape[0])]
    pick_own(column, own_ref, outs)
    add_listed(column, rims_ref, own_ref.shape[2], outs)


def add_pairs(table, blocks, upsample_ref, normal_ref, tangent_ref, rotated_ref, grains, tile, pause=None):
    nodes, width = upsample_ref.shape
    rows = table.shape[0]
    step = padded(width)
    frame = [table[:, i : i + 1] for i in range(9)]
    stacked = jnp.concatenate([ref[:, d * step : d * step + width] for d in range(3) for ref in blocks], axis=0)

    def evaluate(begin, size):
        found = lax.dot_general(stacked, upsample_ref[pl.ds(begin, size), :], NT, preferred_element_type=F32)
        values = [found[d * rows : (d + 1) * rows].astype(BF16).astype(F32) for d in range(3)]
        for c in range(3):
            turned = frame[3 * c] * values[0] + frame[3 * c + 1] * values[1] + frame[3 * c + 2] * values[2]
            rotated_ref[c * rows : (c + 1) * rows, pl.ds(begin, size)] = turned.astype(BF16)

    if tile >= 1024:
        for begin in range(0, nodes, tile):
            evaluate(begin, min(tile, nodes - begin))
    else:

        def body(i, carry):
            evaluate(pl.multiple_of(i * tile, tile), tile)
            return carry

        lax.fori_loop(0, nodes // tile, body, 0)
        if nodes % tile:
            evaluate(nodes // tile * tile, nodes % tile)
    if pause is not None:
        pause()
    normal = jnp.dot(rotated_ref[:rows], normal_ref[...], preferred_element_type=F32)
    tangent = jnp.dot(rotated_ref[rows : 3 * rows], tangent_ref[...], preferred_element_type=F32)
    quad = [normal, tangent[:rows], tangent[rows:]]
    scaling = table[:, SCALE : SCALE + 1]
    lanes = lax.broadcasted_iota(jnp.int32, (rows, grains), 1).astype(F32)
    spot = jnp.where(lanes == table[:, TARGET_COLUMN : TARGET_COLUMN + 1], 1.0, 0.0).astype(BF16)
    spot = jnp.concatenate([spot, spot], axis=0)
    totals = []
    for c in range(3):
        given = (frame[c] * quad[0] + frame[3 + c] * quad[1] + frame[6 + c] * quad[2]) * scaling
        top = given.astype(BF16)
        rest = (given - top.astype(F32)).astype(BF16)
        totals.append(
            lax.dot_general(jnp.concatenate([top, rest], axis=0), spot, TN, preferred_element_type=F32)
        )
    return totals


def exchange_kernel(
    n_ha, opening, tile, round_ref, tables_ref, mine_ref, send_ref, upsample_ref, normal_ref, tangent_ref, *rest
):
    if opening:
        self_ref, own_ref, *rest = rest
    sum_ref, last_ref, table_ref, near_ref, relay_ref, all_ref, rotated_ref, send_sem, recv_sem = rest
    x, y, h = lax.axis_index("gx"), lax.axis_index("gy"), lax.axis_index("ha")
    right, left = (x, y, lax.rem(h + 1, n_ha)), (x, y, lax.rem(h + n_ha - 1, n_ha))
    count = mine_ref.shape[0]
    grains = sum_ref.shape[2]
    half = relay_ref.shape[1]
    upper, lower = pl.ds(0, half), pl.ds(half, count - half)
    lesser = pl.ds(0, count - half)
    barrier = pltpu.get_barrier_semaphore()
    for device in (right, left):
        pl.semaphore_signal(barrier, inc=1, device_id=device, device_id_type=MESH)
    pl.semaphore_wait(barrier, 2)

    def send(source, landing, device, slot):
        copy = pltpu.make_async_remote_copy(
            src_ref=source,
            dst_ref=landing,
            send_sem=send_sem.at[slot],
            recv_sem=recv_sem.at[slot],
            device_id=device,
            device_id_type=MESH,
        )
        copy.start()
        return copy

    direct = [
        send(send_ref.at[0], near_ref.at[0], right, 2),
        send(send_ref.at[2], near_ref.at[1], left, 3),
    ]

    first = (round_ref[0] * count).astype(F32)
    from_place, to_place = table_row(tables_ref, SOURCE_PLACE), table_row(tables_ref, TARGET_PLACE)
    every = jnp.concatenate([tables_ref[j] for j in range(n_ha)], axis=1)
    high = every.astype(BF16)
    middle = (every - high.astype(F32)).astype(BF16)
    low = (every - high.astype(F32) - middle.astype(F32)).astype(BF16)
    parts = jnp.concatenate([high, middle, low], axis=0)
    here = h.astype(F32)
    for place, j in enumerate((0, 1, 3, 2)):
        there = lax.rem(h + n_ha - j, n_ha).astype(F32)
        select = chosen(from_place, to_place, there, here, first, count).astype(BF16)
        found = lax.dot_general(select, parts, NT, preferred_element_type=F32)
        found = found[:, :TABLE] + found[:, TABLE : 2 * TABLE] + found[:, 2 * TABLE :]
        if j == 2:
            table_ref[...] = found
        else:
            all_ref[place * count : (place + 1) * count, :] = found
    weights = (upsample_ref, normal_ref, tangent_ref, rotated_ref, grains, tile)
    totals = add_pairs(all_ref[:count, :], [mine_ref], *weights)
    for c in range(3):
        total = totals[c]
        if opening:
            total += jnp.dot(self_ref[...], own_ref[c], preferred_element_type=F32)
        sum_ref[c] = total
    for copy in direct:
        copy.wait_send()
    across = [
        send(send_ref.at[1, upper], relay_ref.at[0], right, 0),
        send(send_ref.at[1, lower], relay_ref.at[1, lesser], left, 1),
    ]
    for copy in direct:
        copy.wait_recv()
    onward = []

    def pause():
        across[0].wait_recv()
        onward.append(send(relay_ref.at[0], last_ref.at[upper], right, 4))
        across[1].wait_recv()
        onward.append(send(relay_ref.at[1, lesser], last_ref.at[lower], left, 5))

    totals = add_pairs(all_ref[count:, :], [near_ref.at[0], near_ref.at[1]], *weights, pause)
    for c in range(3):
        sum_ref[c] += totals[c]
    for copy in across:
        copy.wait_send()
    for copy in onward:
        copy.wait()


def close_kernel(tile, sum_ref, last_ref, table_ref, upsample_ref, normal_ref, tangent_ref, *rest):
    *before, out_ref, rotated_ref = rest
    width, grains = sum_ref.shape[1:]
    totals = add_pairs(
        table_ref[...], [last_ref], upsample_ref, normal_ref, tangent_ref, rotated_ref, grains, tile
    )
    for c in range(3):
        total = totals[c] + sum_ref[c]
        if before:
            total += before[0][c * width : (c + 1) * width, 0, :]
        out_ref[c * width : (c + 1) * width, 0, :] = total


def shards(
    sizes,
    density,
    upsample,
    normal_kernel,
    tangent_kernel,
    self_operator,
    rim_list,
    pair_target,
    pair_source,
    pair_weight,
    pair_angles,
    live_count,
):
    places = sizes[2]
    width, grains = density.shape[1], density.shape[4]
    nodes = upsample.shape[0]
    rim = rim_list.shape[-1]
    slots = pair_source.shape[-1]
    span = 3 * padded(width)
    count = CAPACITY
    own = density.reshape(3, width, grains)
    normal, tangent = normal_kernel.T, tangent_kernel.T
    listed, table = pl.pallas_call(
        functools.partial(prepare_kernel, places),
        out_shape=[jax.ShapeDtypeStruct((rim, span), BF16), jax.ShapeDtypeStruct((TABLE, slots), F32)],
        in_specs=[SMEM] + [HBM] * 6,
        out_specs=[VMEM, VMEM],
        scratch_shapes=[
            pltpu.VMEM((1, rim), jnp.int32),
            pltpu.VMEM((1, slots), jnp.int32),
            pltpu.VMEM((1, slots), jnp.int32),
            pltpu.VMEM((1, slots), F32),
            pltpu.VMEM((3, 1, slots), F32),
            pltpu.VMEM((3, width, grains), BF16),
            pltpu.SemaphoreType.DMA((6,)),
        ],
        compiler_params=limit(60),
        name="prepare",
    )(
        live_count.reshape(1),
        rim_list.reshape(1, rim),
        pair_target.reshape(1, slots),
        pair_source.reshape(1, slots),
        pair_weight.reshape(1, slots),
        pair_angles.reshape(3, 1, slots),
        own,
    )
    rims, tables, send, mine, most, *weights = pl.pallas_call(
        functools.partial(gather_kernel, sizes),
        out_shape=[
            jax.ShapeDtypeStruct((9, rim, span), BF16),
            jax.ShapeDtypeStruct((places, TABLE, slots), F32),
            jax.ShapeDtypeStruct((places - 1, count, span), BF16),
            jax.ShapeDtypeStruct((count, span), BF16),
            jax.ShapeDtypeStruct((1, 128), F32),
            jax.ShapeDtypeStruct((nodes, width), BF16),
            jax.ShapeDtypeStruct((nodes, width), BF16),
            jax.ShapeDtypeStruct((nodes, width), BF16),
        ],
        in_specs=[ANY, ANY] + [HBM] * 4,
        out_specs=[VMEM] * 8,
        scratch_shapes=[
            pltpu.VMEM((3, width, grains), BF16),
            pltpu.SemaphoreType.DMA((places + 10,)),
            pltpu.SemaphoreType.DMA((places + 10,)),
            pltpu.SemaphoreType.DMA((2,)),
            pltpu.SemaphoreType.DMA((4,)),
        ],
        compiler_params=limit(24, collective_id=0, has_side_effects=True),
        name="gather",
    )(listed, table, own, upsample, normal, tangent)
    place = lax.axis_index("ha").astype(jnp.int32).reshape(1)

    def route(turn):
        return pl.pallas_call(
            route_kernel,
            out_shape=[
                jax.ShapeDtypeStruct((places - 1, count, span), BF16),
                jax.ShapeDtypeStruct((count, span), BF16),
            ],
            in_specs=[SMEM, SMEM, VMEM, VMEM, VMEM],
            out_specs=[VMEM, VMEM],
            compiler_params=limit(24),
            name="route",
        )(turn, place, tables, own, rims)

    def finish(turn, mine, send, before):
        opening = before is None
        tile = WIDE if opening else NARROW
        held = weights if opening else [upsample, normal, tangent]
        mixed = [self_operator, own] if opening else []
        total, last, rows = pl.pallas_call(
            functools.partial(exchange_kernel, places, opening, tile),
            out_shape=[
                jax.ShapeDtypeStruct((3, width, grains), F32),
                jax.ShapeDtypeStruct((count, span), BF16),
                jax.ShapeDtypeStruct((count, TABLE), F32),
            ],
            in_specs=[SMEM, VMEM, VMEM, ANY] + [VMEM] * (3 + len(mixed)),
            out_specs=[VMEM] * 3,
            scratch_shapes=[
                pltpu.VMEM((2, count, span), BF16),
                pltpu.VMEM((2, (count // 2 + 15) // 16 * 16, span), BF16),
                pltpu.VMEM((3 * count, TABLE), F32),
                pltpu.VMEM((6 * count, nodes), BF16),
                pltpu.SemaphoreType.DMA((6,)),
                pltpu.SemaphoreType.DMA((6,)),
            ],
            compiler_params=limit(30, collective_id=1 if opening else 2, has_side_effects=True),
            name="exchange",
        )(turn, tables, mine, send, *held, *mixed)
        ended = [] if opening else [before]
        return pl.pallas_call(
            functools.partial(close_kernel, tile),
            out_shape=jax.ShapeDtypeStruct((3 * width, 1, grains), F32),
            in_specs=[VMEM] * (6 + len(ended)),
            out_specs=VMEM,
            scratch_shapes=[pltpu.VMEM((3 * count, nodes), BF16)],
            compiler_params=limit(30),
            name="close",
        )(total, last, rows, *held, *ended)

    turn = jnp.zeros((1,), jnp.int32)
    result = finish(turn, mine, send, None)
    result, most = lax.optimization_barrier((result, most))
    rounds = (most[0, 0].astype(jnp.int32) + count - 1) // count

    def again(state):
        now, total = state
        send, mine = route(now.reshape(1))
        return now + 1, finish(now.reshape(1), mine, send, total)

    _, result = lax.while_loop(lambda state: state[0] < rounds, again, (jnp.int32(1), result))
    return result.reshape(3, width, 1, 1, grains)


def solution(mesh):
    sizes = tuple(mesh.shape[axis] for axis in ("gx", "gy", "ha"))
    return jax.shard_map(
        functools.partial(shards, sizes),
        mesh=mesh,
        in_specs=(
            P(None, None, "gx", "gy", "ha"),
            P(),
            P(),
            P(),
            P(),
            P("gx", "gy", "ha"),
            P("gx", "gy", "ha", None),
            P("gx", "gy", "ha", None),
            P("gx", "gy", "ha", None),
            P(None, "gx", "gy", "ha", None),
            P("gx", "gy", "ha"),
        ),
        out_specs=P(None, None, "gx", "gy", "ha"),
        check_vma=False,
    )
```

```python
import functools

import jax
import jax.numpy as jnp
from jax import lax
from jax.experimental import pallas as pl
from jax.experimental.pallas import tpu as pltpu
from jax.sharding import PartitionSpec as P

MESH = pl.DeviceIdType.MESH
ANY = pl.BlockSpec(memory_space=pl.ANY)
VMEM = pl.BlockSpec(memory_space=pltpu.VMEM)
SMEM = pl.BlockSpec(memory_space=pltpu.SMEM)
HBM = pl.BlockSpec(memory_space=pltpu.HBM)
CAPACITY = 88
WIDE, NARROW = 1152, 256
TABLE = 16
SCALE, SOURCE_PLACE, SOURCE_COLUMN, TARGET_PLACE, TARGET_COLUMN = 9, 10, 11, 12, 13
NT = (((1,), (1,)), ((), ()))
TN = (((0,), (0,)), ((), ()))
F32 = jnp.float32
BF16 = jnp.bfloat16


def padded(width):
    return (width + 127) // 128 * 128


def limit(mebibytes, **others):
    return pltpu.CompilerParams(vmem_limit_bytes=mebibytes * 1024 * 1024, **others)


def split(value, size):
    bits = size.bit_length() - 1
    assert size == 1 << bits
    return lax.shift_right_logical(value, bits), value & (size - 1)


def load(sources, landings, sem):
    copies = [pltpu.make_async_copy(a, b, sem.at[i]) for i, (a, b) in enumerate(zip(sources, landings))]
    for copy in copies:
        copy.start()
    return copies


def prepare_kernel(
    places, live_ref, list_hbm, target_hbm, source_hbm, weight_hbm, angles_hbm, own_hbm, packed_ref,
    list_ref, target_ref, source_ref, weight_ref, angles_ref, own_ref, sem,
):
    loads = load(
        [list_hbm, target_hbm, source_hbm, weight_hbm, angles_hbm, own_hbm],
        [list_ref, target_ref, source_ref, weight_ref, angles_ref, own_ref],
        sem,
    )
    packed_ref[...] = jnp.zeros_like(packed_ref)
    width, grains = own_ref.shape[1:]
    rim, slots = list_ref.shape[1], source_ref.shape[1]
    step = padded(width)
    for copy in loads[:5]:
        copy.wait()
    angles = jnp.concatenate([angles_ref[i] for i in range(3)], axis=0)
    cosines, sines = jnp.cos(angles), jnp.sin(angles)
    c0, c1, c2 = (cosines[i : i + 1] for i in range(3))
    s0, s1, s2 = (sines[i : i + 1] for i in range(3))
    frame = [
        c0 * c1 * c2 - s0 * s2, -(c0 * c1 * s2) - s0 * c2, c0 * s1,
        s0 * c1 * c2 + c0 * s2, -(s0 * c1 * s2) + c0 * c2, s0 * s1,
        -(s1 * c2), s1 * s2, c1,
    ]
    alive = lax.broadcasted_iota(jnp.int32, (1, slots), 1) < live_ref[0]
    source = source_ref[...]
    inside = source < grains * places
    place, column = split(source, grains)
    group, within = split(jnp.maximum(source - grains * places, 0), rim * places)
    rim_place, rim_column = split(within, rim)
    target_place, target_column = split(target_ref[...], grains)
    rows = frame + [
        jnp.where(alive, weight_ref[...], 0.0),
        jnp.where(inside, place, rim_place).astype(F32),
        jnp.where(inside, column, grains + group * rim + rim_column).astype(F32),
        jnp.where(alive, target_place, -1).astype(F32),
        target_column.astype(F32),
    ]
    rows += [jnp.zeros((1, slots), F32)] * (TABLE - len(rows))
    table = jnp.concatenate(rows, axis=0)
    high = table.astype(BF16)
    middle = (table - high.astype(F32)).astype(BF16)
    low = (table - high.astype(F32) - middle.astype(F32)).astype(BF16)
    for i, part in enumerate((high, middle, low)):
        packed_ref[rim : rim + TABLE, i * slots : (i + 1) * slots] = part
    square = [lax.broadcasted_iota(jnp.int32, (rim, rim), axis) for axis in (0, 1)]
    listed = jnp.where(square[0] == square[1], list_ref[...].astype(F32), 0.0)
    listed = jnp.sum(listed, axis=1, keepdims=True)
    lanes = lax.broadcasted_iota(jnp.int32, (rim, grains), 1).astype(F32)
    pick = jnp.where(listed == lanes, 1.0, 0.0).astype(BF16)
    loads[5].wait()
    for c in range(3):
        found = lax.dot_general(pick, own_ref[c], NT, preferred_element_type=F32)
        packed_ref[:rim, c * step : c * step + width] = found.astype(BF16)


def gather_kernel(
    sizes, packed_ref, own_hbm, upsample_hbm, normal_hbm, tangent_hbm,
    rims_ref, tables_ref, send_ref, mine_ref, most_ref, upsample_ref, normal_ref, tangent_ref,
    own_ref, send_sem, recv_sem, own_sem, load_sem,
):
    n_gx, n_gy, n_ha = sizes
    rim_ref = packed_ref.at[pl.ds(0, rims_ref.shape[1])]
    table_ref = packed_ref.at[pl.ds(rims_ref.shape[1], TABLE), pl.ds(0, tables_ref.shape[2])]
    x, y, h = lax.axis_index("gx"), lax.axis_index("gy"), lax.axis_index("ha")
    loads = load(
        [own_hbm, upsample_hbm, normal_hbm, tangent_hbm],
        [own_ref, upsample_ref, normal_ref, tangent_ref],
        load_sem,
    )
    near = 1 - 2 * lax.rem(y, 2)
    partner = (x, y + near, h)
    far = lax.rem(y - near + n_gy, n_gy)
    barrier = pltpu.get_barrier_semaphore()
    mates = [(x, y, lax.rem(h + j, n_ha)) for j in range(1, n_ha)]
    sides = [(lax.rem(x + dx + n_gx, n_gx), y, h) for dx in (-1, 1)]
    beyond = [(lax.rem(x + dx + n_gx, n_gx), far, h) for dx in (-1, 1)]
    ahead = (x, far, h)
    relays = lax.rem(x, 2) == lax.rem(y, 2)
    peers = mates + sides + beyond + [ahead, partner]
    for device in peers:
        pl.semaphore_signal(barrier, inc=1, device_id=device, device_id_type=MESH)
    own = [
        pltpu.make_async_copy(rim_ref, rims_ref.at[4], own_sem.at[0]),
        pltpu.make_async_copy(table_ref, tables_ref.at[h], own_sem.at[1]),
    ]
    for copy in own:
        copy.start()
    pl.semaphore_wait(barrier, len(peers))

    def send(source, landing, device, leaving, arriving):
        return pltpu.make_async_remote_copy(
            src_ref=source,
            dst_ref=landing,
            send_sem=send_sem.at[leaving],
            recv_sem=recv_sem.at[arriving],
            device_id=device,
            device_id_type=MESH,
        )

    tables = [send(table_ref, tables_ref.at[h], mates[j], j, j) for j in range(n_ha - 1)]
    for copy in tables:
        copy.start()
    aside, middle, onward, wide, across = [], [], [], [], []
    for i, dx in enumerate((-1, 1)):
        column, away = (dx + 1) * 3 + 1, (1 - dx) * 3 + 1
        aside.append(send(rim_ref, rims_ref.at[away], sides[i], n_ha + i, n_ha + 1 - i))
        onward.append(send(rims_ref.at[column], rims_ref.at[column - near], partner, n_ha + 2 + i, n_ha + 2 + i))
        across.append(send(rims_ref.at[column], rims_ref.at[column + near], ahead, n_ha + 4 + i, n_ha + 8 + i))
        wide.append(send(rim_ref, rims_ref.at[away + near], beyond[i], n_ha + 6 + i, n_ha + 9 - i))
    middle = [
        send(rim_ref, rims_ref.at[4 - near], partner, n_ha + 8, n_ha + 4),
        send(rim_ref, rims_ref.at[4 + near], ahead, n_ha + 9, n_ha + 5),
    ]
    for copy in aside + middle:
        copy.start()

    @pl.when(relays)
    def _():
        for copy in wide:
            copy.start()

    loads[0].wait()
    for copy in own:
        copy.wait()
    for copy in tables:
        copy.wait()
    column = route_columns(jnp.float32(0.0), h, tables_ref, mine_ref.shape[0])
    outs = [mine_ref] + [send_ref.at[j] for j in range(n_ha - 1)]
    pick_own(column, own_ref, outs)
    most_ref[...] = jnp.broadcast_to(longest(tables_ref), most_ref.shape)
    for copy in aside:
        copy.wait_recv()
    for copy in onward:
        copy.start()

    @pl.when(relays)
    def _():
        for copy in across:
            copy.start()

    for copy in loads[1:]:
        copy.wait()
    for copy in aside:
        copy.wait_send()
    for copy in middle + onward:
        copy.wait()
    for copy in across:
        copy.wait_recv()

    @pl.when(relays)
    def _():
        for copy in wide + across:
            copy.wait_send()

    add_listed(column, rims_ref, own_ref.shape[2], outs)


def ranks(mask):
    total, length = mask, mask.shape[1]
    lanes = lax.broadcasted_iota(jnp.int32, mask.shape, 1)
    step = 1
    while step < length:
        total = total + jnp.where(lanes >= step, pltpu.roll(total, step, 1), 0.0)
        step *= 2
    return total - mask


def table_parts(tables_ref):
    places, slots = tables_ref.shape[0], tables_ref.shape[2] // 3
    return [
        jnp.concatenate([tables_ref[j, :, i * slots : (i + 1) * slots] for j in range(places)], axis=1)
        for i in range(3)
    ]


def table_places(tables_ref):
    high, middle, _ = (part.astype(F32) for part in table_parts(tables_ref))
    whole = high + middle
    return [whole[i : i + 1] for i in (SOURCE_PLACE, TARGET_PLACE, SOURCE_COLUMN)]


def chosen(from_place, to_place, source, target, first, count):
    mask = jnp.where((from_place == source) & (to_place == target), 1.0, 0.0)
    key = jnp.where(mask > 0.0, ranks(mask) - first, -1.0)
    rows = lax.broadcasted_iota(jnp.int32, (count, mask.shape[1]), 0).astype(F32)
    return jnp.where(rows == key, 1.0, 0.0)


def route_columns(first, place, tables_ref, count):
    places = tables_ref.shape[0]
    here = place.astype(F32)
    from_place, to_place, column_row = table_places(tables_ref)
    column_row = column_row + 1.0
    columns = []
    for j in range(places):
        there = lax.rem(place + j, places).astype(F32)
        select = chosen(from_place, to_place, here, there, first, count)
        columns.append(jnp.sum(select * column_row, axis=1, keepdims=True) - 1.0)
    return jnp.concatenate(columns, axis=0)


def longest(tables_ref):
    places = tables_ref.shape[0]
    from_place, to_place, _ = table_places(tables_ref)
    most = jnp.zeros((1, 1), F32)
    for source in range(places):
        for target in range(places):
            hit = jnp.where((from_place == float(source)) & (to_place == float(target)), 1.0, 0.0)
            most = jnp.maximum(most, jnp.sum(hit, axis=1, keepdims=True))
    return most


def pick_own(column, own_ref, outs):
    rows, (width, grains) = column.shape[0], own_ref.shape[1:]
    step, count = padded(width), outs[0].shape[0]
    lanes = lax.broadcasted_iota(jnp.int32, (rows, grains), 1).astype(F32)
    pick = jnp.where(lanes == column, 1.0, 0.0).astype(BF16)
    for out in outs:
        out[...] = jnp.zeros(out.shape, BF16)
    for c in range(3):
        found = lax.dot_general(pick, own_ref[c], NT, preferred_element_type=F32)
        for j, out in enumerate(outs):
            out[:, c * step : c * step + width] = found[j * count : (j + 1) * count].astype(BF16)


def add_listed(column, rims_ref, grains, outs):
    rows, groups, rim = column.shape[0], rims_ref.shape[0], rims_ref.shape[1]
    span, count = rims_ref.shape[2], outs[0].shape[0]
    lanes = lax.broadcasted_iota(jnp.int32, (rows, groups * rim), 1).astype(F32) + float(grains)
    pick = jnp.where(lanes == column, 1.0, 0.0).astype(BF16)
    for begin in range(0, span, span // 3):
        part = slice(begin, begin + span // 3)
        rims = rims_ref[:, :, part].reshape(groups * rim, span // 3)
        found = jnp.dot(pick, rims, preferred_element_type=F32)
        for j, out in enumerate(outs):
            out[:, part] = (out[:, part].astype(F32) + found[j * count : (j + 1) * count]).astype(BF16)


def route_kernel(round_ref, place_ref, tables_ref, own_ref, rims_ref, send_ref, mine_ref):
    count = mine_ref.shape[0]
    column = route_columns((round_ref[0] * count).astype(F32), place_ref[0], tables_ref, count)
    outs = [mine_ref] + [send_ref.at[j] for j in range(send_ref.shape[0])]
    pick_own(column, own_ref, outs)
    add_listed(column, rims_ref, own_ref.shape[2], outs)


def add_pairs(table, blocks, upsample_ref, normal_ref, tangent_ref, rotated_ref, grains, tile, pause=None):
    nodes, width = upsample_ref.shape
    rows = table.shape[0]
    step = padded(width)
    frame = [table[:, i : i + 1] for i in range(9)]
    stacked = jnp.concatenate([ref[:, d * step : d * step + width] for d in range(3) for ref in blocks], axis=0)

    def evaluate(begin, size):
        found = lax.dot_general(stacked, upsample_ref[pl.ds(begin, size), :], NT, preferred_element_type=F32)
        values = [found[d * rows : (d + 1) * rows].astype(BF16).astype(F32) for d in range(3)]
        for c in range(3):
            turned = frame[3 * c] * values[0] + frame[3 * c + 1] * values[1] + frame[3 * c + 2] * values[2]
            rotated_ref[c * rows : (c + 1) * rows, pl.ds(begin, size)] = turned.astype(BF16)

    if tile >= 1024:
        for begin in range(0, nodes, tile):
            evaluate(begin, min(tile, nodes - begin))
    else:

        def body(i, carry):
            evaluate(pl.multiple_of(i * tile, tile), tile)
            return carry

        lax.fori_loop(0, nodes // tile, body, 0)
        if nodes % tile:
            evaluate(nodes // tile * tile, nodes % tile)
    if pause is not None:
        pause()
    normal = jnp.dot(rotated_ref[:rows], normal_ref[...], preferred_element_type=F32)
    tangent = jnp.dot(rotated_ref[rows : 3 * rows], tangent_ref[...], preferred_element_type=F32)
    quad = [normal, tangent[:rows], tangent[rows:]]
    scaling = table[:, SCALE : SCALE + 1]
    lanes = lax.broadcasted_iota(jnp.int32, (rows, grains), 1).astype(F32)
    spot = jnp.where(lanes == table[:, TARGET_COLUMN : TARGET_COLUMN + 1], 1.0, 0.0).astype(BF16)
    spot = jnp.concatenate([spot, spot], axis=0)
    totals = []
    for c in range(3):
        given = (frame[c] * quad[0] + frame[3 + c] * quad[1] + frame[6 + c] * quad[2]) * scaling
        top = given.astype(BF16)
        rest = (given - top.astype(F32)).astype(BF16)
        totals.append(
            lax.dot_general(jnp.concatenate([top, rest], axis=0), spot, TN, preferred_element_type=F32)
        )
    return totals


def exchange_kernel(
    n_ha, opening, tile, round_ref, tables_ref, mine_ref, send_ref, upsample_ref, normal_ref, tangent_ref, *rest
):
    if opening:
        self_ref, own_ref, *rest = rest
    sum_ref, last_ref, table_ref, near_ref, relay_ref, all_ref, rotated_ref, send_sem, recv_sem = rest
    x, y, h = lax.axis_index("gx"), lax.axis_index("gy"), lax.axis_index("ha")
    right, left = (x, y, lax.rem(h + 1, n_ha)), (x, y, lax.rem(h + n_ha - 1, n_ha))
    count = mine_ref.shape[0]
    grains = sum_ref.shape[2]
    half = relay_ref.shape[1]
    upper, lower = pl.ds(0, half), pl.ds(half, count - half)
    lesser = pl.ds(0, count - half)
    barrier = pltpu.get_barrier_semaphore()
    for device in (right, left):
        pl.semaphore_signal(barrier, inc=1, device_id=device, device_id_type=MESH)
    pl.semaphore_wait(barrier, 2)

    def send(source, landing, device, slot):
        copy = pltpu.make_async_remote_copy(
            src_ref=source,
            dst_ref=landing,
            send_sem=send_sem.at[slot],
            recv_sem=recv_sem.at[slot],
            device_id=device,
            device_id_type=MESH,
        )
        copy.start()
        return copy

    direct = [
        send(send_ref.at[0], near_ref.at[0], right, 2),
        send(send_ref.at[2], near_ref.at[1], left, 3),
    ]

    first = (round_ref[0] * count).astype(F32)
    from_place, to_place, _ = table_places(tables_ref)
    parts = jnp.concatenate(table_parts(tables_ref), axis=0)
    here = h.astype(F32)
    for place, j in enumerate((0, 1, 3, 2)):
        there = lax.rem(h + n_ha - j, n_ha).astype(F32)
        select = chosen(from_place, to_place, there, here, first, count).astype(BF16)
        found = lax.dot_general(select, parts, NT, preferred_element_type=F32)
        found = found[:, :TABLE] + found[:, TABLE : 2 * TABLE] + found[:, 2 * TABLE :]
        if j == 2:
            table_ref[...] = found
        else:
            all_ref[place * count : (place + 1) * count, :] = found
    weights = (upsample_ref, normal_ref, tangent_ref, rotated_ref, grains, tile)
    totals = add_pairs(all_ref[:count, :], [mine_ref], *weights)
    for c in range(3):
        total = totals[c]
        if opening:
            total += jnp.dot(self_ref[...], own_ref[c], preferred_element_type=F32)
        sum_ref[c] = total
    for copy in direct:
        copy.wait_send()
    across = [
        send(send_ref.at[1, upper], relay_ref.at[0], right, 0),
        send(send_ref.at[1, lower], relay_ref.at[1, lesser], left, 1),
    ]
    for copy in direct:
        copy.wait_recv()
    onward = []

    def pause():
        across[0].wait_recv()
        onward.append(send(relay_ref.at[0], last_ref.at[upper], right, 4))
        across[1].wait_recv()
        onward.append(send(relay_ref.at[1, lesser], last_ref.at[lower], left, 5))

    totals = add_pairs(all_ref[count:, :], [near_ref.at[0], near_ref.at[1]], *weights, pause)
    for c in range(3):
        sum_ref[c] += totals[c]
    for copy in across:
        copy.wait_send()
    for copy in onward:
        copy.wait()


def close_kernel(tile, sum_ref, last_ref, table_ref, upsample_ref, normal_ref, tangent_ref, *rest):
    *before, out_ref, rotated_ref = rest
    width, grains = sum_ref.shape[1:]
    totals = add_pairs(
        table_ref[...], [last_ref], upsample_ref, normal_ref, tangent_ref, rotated_ref, grains, tile
    )
    for c in range(3):
        total = totals[c] + sum_ref[c]
        if before:
            total += before[0][c * width : (c + 1) * width, 0, :]
        out_ref[c * width : (c + 1) * width, 0, :] = total


def shards(
    sizes,
    density,
    upsample,
    normal_kernel,
    tangent_kernel,
    self_operator,
    rim_list,
    pair_target,
    pair_source,
    pair_weight,
    pair_angles,
    live_count,
):
    places = sizes[2]
    width, grains = density.shape[1], density.shape[4]
    nodes = upsample.shape[0]
    rim = rim_list.shape[-1]
    slots = pair_source.shape[-1]
    span = 3 * padded(width)
    count = CAPACITY
    own = density.reshape(3, width, grains)
    normal, tangent = normal_kernel.T, tangent_kernel.T
    packed = pl.pallas_call(
        functools.partial(prepare_kernel, places),
        out_shape=jax.ShapeDtypeStruct((rim + TABLE, span), BF16),
        in_specs=[SMEM] + [HBM] * 6,
        out_specs=VMEM,
        scratch_shapes=[
            pltpu.VMEM((1, rim), jnp.int32),
            pltpu.VMEM((1, slots), jnp.int32),
            pltpu.VMEM((1, slots), jnp.int32),
            pltpu.VMEM((1, slots), F32),
            pltpu.VMEM((3, 1, slots), F32),
            pltpu.VMEM((3, width, grains), BF16),
            pltpu.SemaphoreType.DMA((6,)),
        ],
        compiler_params=limit(60),
        name="prepare",
    )(
        live_count.reshape(1),
        rim_list.reshape(1, rim),
        pair_target.reshape(1, slots),
        pair_source.reshape(1, slots),
        pair_weight.reshape(1, slots),
        pair_angles.reshape(3, 1, slots),
        own,
    )
    rims, tables, send, mine, most, *weights = pl.pallas_call(
        functools.partial(gather_kernel, sizes),
        out_shape=[
            jax.ShapeDtypeStruct((9, rim, span), BF16),
            jax.ShapeDtypeStruct((places, TABLE, 3 * slots), BF16),
            jax.ShapeDtypeStruct((places - 1, count, span), BF16),
            jax.ShapeDtypeStruct((count, span), BF16),
            jax.ShapeDtypeStruct((1, 128), F32),
            jax.ShapeDtypeStruct((nodes, width), BF16),
            jax.ShapeDtypeStruct((nodes, width), BF16),
            jax.ShapeDtypeStruct((nodes, width), BF16),
        ],
        in_specs=[ANY] + [HBM] * 4,
        out_specs=[VMEM] * 8,
        scratch_shapes=[
            pltpu.VMEM((3, width, grains), BF16),
            pltpu.SemaphoreType.DMA((places + 10,)),
            pltpu.SemaphoreType.DMA((places + 10,)),
            pltpu.SemaphoreType.DMA((2,)),
            pltpu.SemaphoreType.DMA((4,)),
        ],
        compiler_params=limit(24, collective_id=0, has_side_effects=True),
        name="gather",
    )(packed, own, upsample, normal, tangent)
    place = lax.axis_index("ha").astype(jnp.int32).reshape(1)

    def route(turn):
        return pl.pallas_call(
            route_kernel,
            out_shape=[
                jax.ShapeDtypeStruct((places - 1, count, span), BF16),
                jax.ShapeDtypeStruct((count, span), BF16),
            ],
            in_specs=[SMEM, SMEM, VMEM, VMEM, VMEM],
            out_specs=[VMEM, VMEM],
            compiler_params=limit(24),
            name="route",
        )(turn, place, tables, own, rims)

    def finish(turn, mine, send, before):
        opening = before is None
        tile = WIDE if opening else NARROW
        held = weights if opening else [upsample, normal, tangent]
        mixed = [self_operator, own] if opening else []
        total, last, rows = pl.pallas_call(
            functools.partial(exchange_kernel, places, opening, tile),
            out_shape=[
                jax.ShapeDtypeStruct((3, width, grains), F32),
                jax.ShapeDtypeStruct((count, span), BF16),
                jax.ShapeDtypeStruct((count, TABLE), F32),
            ],
            in_specs=[SMEM, VMEM, VMEM, ANY] + [VMEM] * (3 + len(mixed)),
            out_specs=[VMEM] * 3,
            scratch_shapes=[
                pltpu.VMEM((2, count, span), BF16),
                pltpu.VMEM((2, (count // 2 + 15) // 16 * 16, span), BF16),
                pltpu.VMEM((3 * count, TABLE), F32),
                pltpu.VMEM((6 * count, nodes), BF16),
                pltpu.SemaphoreType.DMA((6,)),
                pltpu.SemaphoreType.DMA((6,)),
            ],
            compiler_params=limit(30, collective_id=1 if opening else 2, has_side_effects=True),
            name="exchange",
        )(turn, tables, mine, send, *held, *mixed)
        ended = [] if opening else [before]
        return pl.pallas_call(
            functools.partial(close_kernel, tile),
            out_shape=jax.ShapeDtypeStruct((3 * width, 1, grains), F32),
            in_specs=[VMEM] * (6 + len(ended)),
            out_specs=VMEM,
            scratch_shapes=[pltpu.VMEM((3 * count, nodes), BF16)],
            compiler_params=limit(30),
            name="close",
        )(total, last, rows, *held, *ended)

    turn = jnp.zeros((1,), jnp.int32)
    result = finish(turn, mine, send, None)
    result, most = lax.optimization_barrier((result, most))
    rounds = (most[0, 0].astype(jnp.int32) + count - 1) // count

    def again(state):
        now, total = state
        send, mine = route(now.reshape(1))
        return now + 1, finish(now.reshape(1), mine, send, total)

    _, result = lax.while_loop(lambda state: state[0] < rounds, again, (jnp.int32(1), result))
    return result.reshape(3, width, 1, 1, grains)


def solution(mesh):
    sizes = tuple(mesh.shape[axis] for axis in ("gx", "gy", "ha"))
    return jax.shard_map(
        functools.partial(shards, sizes),
        mesh=mesh,
        in_specs=(
            P(None, None, "gx", "gy", "ha"),
            P(),
            P(),
            P(),
            P(),
            P("gx", "gy", "ha"),
            P("gx", "gy", "ha", None),
            P("gx", "gy", "ha", None),
            P("gx", "gy", "ha", None),
            P(None, "gx", "gy", "ha", None),
            P("gx", "gy", "ha"),
        ),
        out_specs=P(None, None, "gx", "gy", "ha"),
        check_vma=False,
    )
```

```python
import functools

import jax
import jax.numpy as jnp
from jax import lax
from jax.experimental import pallas as pl
from jax.experimental.pallas import tpu as pltpu
from jax.sharding import PartitionSpec as P

MESH = pl.DeviceIdType.MESH
ANY = pl.BlockSpec(memory_space=pl.ANY)
VMEM = pl.BlockSpec(memory_space=pltpu.VMEM)
SMEM = pl.BlockSpec(memory_space=pltpu.SMEM)
HBM = pl.BlockSpec(memory_space=pltpu.HBM)
CAPACITY = 88
WIDE, NARROW = 1152, 256
TABLE = 16
SCALE, SOURCE_PLACE, SOURCE_COLUMN, TARGET_PLACE, TARGET_COLUMN = 9, 10, 11, 12, 13
NT = (((1,), (1,)), ((), ()))
TN = (((0,), (0,)), ((), ()))
F32 = jnp.float32
BF16 = jnp.bfloat16


def padded(width):
    return (width + 127) // 128 * 128


def limit(mebibytes, **others):
    return pltpu.CompilerParams(vmem_limit_bytes=mebibytes * 1024 * 1024, **others)


def split(value, size):
    bits = size.bit_length() - 1
    assert size == 1 << bits
    return lax.shift_right_logical(value, bits), value & (size - 1)


def load(sources, landings, sem):
    copies = [pltpu.make_async_copy(a, b, sem.at[i]) for i, (a, b) in enumerate(zip(sources, landings))]
    for copy in copies:
        copy.start()
    return copies


def prepare_kernel(
    places, live_ref, list_hbm, target_hbm, source_hbm, weight_hbm, angles_hbm, own_hbm, packed_ref,
    list_ref, target_ref, source_ref, weight_ref, angles_ref, own_ref, sem,
):
    loads = load(
        [list_hbm, target_hbm, source_hbm, weight_hbm, angles_hbm, own_hbm],
        [list_ref, target_ref, source_ref, weight_ref, angles_ref, own_ref],
        sem,
    )
    packed_ref[...] = jnp.zeros_like(packed_ref)
    width, grains = own_ref.shape[1:]
    rim, slots = list_ref.shape[1], source_ref.shape[1]
    step = padded(width)
    for copy in loads[:5]:
        copy.wait()
    angles = jnp.concatenate([angles_ref[i] for i in range(3)], axis=0)
    cosines, sines = jnp.cos(angles), jnp.sin(angles)
    c0, c1, c2 = (cosines[i : i + 1] for i in range(3))
    s0, s1, s2 = (sines[i : i + 1] for i in range(3))
    frame = [
        c0 * c1 * c2 - s0 * s2, -(c0 * c1 * s2) - s0 * c2, c0 * s1,
        s0 * c1 * c2 + c0 * s2, -(s0 * c1 * s2) + c0 * c2, s0 * s1,
        -(s1 * c2), s1 * s2, c1,
    ]
    alive = lax.broadcasted_iota(jnp.int32, (1, slots), 1) < live_ref[0]
    source = source_ref[...]
    inside = source < grains * places
    place, column = split(source, grains)
    group, within = split(jnp.maximum(source - grains * places, 0), rim * places)
    rim_place, rim_column = split(within, rim)
    target_place, target_column = split(target_ref[...], grains)
    rows = frame + [
        jnp.where(alive, weight_ref[...], 0.0),
        jnp.where(inside, place, rim_place).astype(F32),
        jnp.where(inside, column, grains + group * rim + rim_column).astype(F32),
        jnp.where(alive, target_place, -1).astype(F32),
        target_column.astype(F32),
    ]
    rows += [jnp.zeros((1, slots), F32)] * (TABLE - len(rows))
    table = jnp.concatenate(rows, axis=0)
    high = table.astype(BF16)
    middle = (table - high.astype(F32)).astype(BF16)
    low = (table - high.astype(F32) - middle.astype(F32)).astype(BF16)
    for i, part in enumerate((high, middle, low)):
        packed_ref[rim : rim + TABLE, i * slots : (i + 1) * slots] = part
    square = [lax.broadcasted_iota(jnp.int32, (rim, rim), axis) for axis in (0, 1)]
    listed = jnp.where(square[0] == square[1], list_ref[...].astype(F32), 0.0)
    listed = jnp.sum(listed, axis=1, keepdims=True)
    lanes = lax.broadcasted_iota(jnp.int32, (rim, grains), 1).astype(F32)
    pick = jnp.where(listed == lanes, 1.0, 0.0).astype(BF16)
    loads[5].wait()
    for c in range(3):
        found = lax.dot_general(pick, own_ref[c], NT, preferred_element_type=F32)
        packed_ref[:rim, c * step : c * step + width] = found.astype(BF16)


def gather_kernel(
    sizes, packed_ref, own_hbm, upsample_hbm, normal_hbm, tangent_hbm,
    rims_ref, tables_ref, send_ref, mine_ref, most_ref, upsample_ref, normal_ref, tangent_ref,
    own_ref, send_sem, recv_sem, own_sem, load_sem,
):
    n_gx, n_gy, n_ha = sizes
    rim_ref = packed_ref.at[pl.ds(0, rims_ref.shape[1])]
    table_ref = packed_ref.at[pl.ds(rims_ref.shape[1], TABLE), pl.ds(0, tables_ref.shape[2])]
    x, y, h = lax.axis_index("gx"), lax.axis_index("gy"), lax.axis_index("ha")
    loads = load(
        [own_hbm, upsample_hbm, normal_hbm, tangent_hbm],
        [own_ref, upsample_ref, normal_ref, tangent_ref],
        load_sem,
    )
    near = 1 - 2 * lax.rem(y, 2)
    partner = (x, y + near, h)
    far = lax.rem(y - near + n_gy, n_gy)
    barrier = pltpu.get_barrier_semaphore()
    mates = [(x, y, lax.rem(h + j, n_ha)) for j in range(1, n_ha)]
    sides = [(lax.rem(x + dx + n_gx, n_gx), y, h) for dx in (-1, 1)]
    beyond = [(lax.rem(x + dx + n_gx, n_gx), far, h) for dx in (-1, 1)]
    ahead = (x, far, h)
    relays = lax.rem(x, 2) == lax.rem(y, 2)
    peers = mates + sides + beyond + [ahead, partner]
    for device in peers:
        pl.semaphore_signal(barrier, inc=1, device_id=device, device_id_type=MESH)
    own = [
        pltpu.make_async_copy(rim_ref, rims_ref.at[4], own_sem.at[0]),
        pltpu.make_async_copy(table_ref, tables_ref.at[h], own_sem.at[1]),
    ]
    for copy in own:
        copy.start()
    pl.semaphore_wait(barrier, len(peers))

    def send(source, landing, device, leaving, arriving):
        return pltpu.make_async_remote_copy(
            src_ref=source,
            dst_ref=landing,
            send_sem=send_sem.at[leaving],
            recv_sem=recv_sem.at[arriving],
            device_id=device,
            device_id_type=MESH,
        )

    tables = [send(table_ref, tables_ref.at[h], mates[j], j, j) for j in range(n_ha - 1)]
    for copy in tables:
        copy.start()
    aside, middle, onward, wide, across = [], [], [], [], []
    for i, dx in enumerate((-1, 1)):
        column, away = (dx + 1) * 3 + 1, (1 - dx) * 3 + 1
        aside.append(send(rim_ref, rims_ref.at[away], sides[i], n_ha + i, n_ha + 1 - i))
        onward.append(send(rims_ref.at[column], rims_ref.at[column - near], partner, n_ha + 2 + i, n_ha + 2 + i))
        across.append(send(rims_ref.at[column], rims_ref.at[column + near], ahead, n_ha + 4 + i, n_ha + 8 + i))
        wide.append(send(rim_ref, rims_ref.at[away + near], beyond[i], n_ha + 6 + i, n_ha + 9 - i))
    middle = [
        send(rim_ref, rims_ref.at[4 - near], partner, n_ha + 8, n_ha + 4),
        send(rim_ref, rims_ref.at[4 + near], ahead, n_ha + 9, n_ha + 5),
    ]
    for copy in aside + middle:
        copy.start()

    @pl.when(relays)
    def _():
        for copy in wide:
            copy.start()

    loads[0].wait()
    for copy in own:
        copy.wait()
    for copy in tables:
        copy.wait()
    column = route_columns(jnp.float32(0.0), h, tables_ref, mine_ref.shape[0])
    outs = [mine_ref] + [send_ref.at[j] for j in range(n_ha - 1)]
    pick_own(column, own_ref, outs)
    most_ref[...] = jnp.broadcast_to(longest(tables_ref), most_ref.shape)
    for copy in aside:
        copy.wait_recv()
    for copy in onward:
        copy.start()

    @pl.when(relays)
    def _():
        for copy in across:
            copy.start()

    for copy in loads[1:]:
        copy.wait()
    for copy in aside:
        copy.wait_send()
    for copy in middle + onward:
        copy.wait()
    for copy in across:
        copy.wait_recv()

    @pl.when(relays)
    def _():
        for copy in wide + across:
            copy.wait_send()

    add_listed(column, rims_ref, own_ref.shape[2], outs)


def ranks(mask):
    total, length = mask, mask.shape[1]
    lanes = lax.broadcasted_iota(jnp.int32, mask.shape, 1)
    step = 1
    while step < length:
        total = total + jnp.where(lanes >= step, pltpu.roll(total, step, 1), 0.0)
        step *= 2
    return total - mask


def table_parts(tables_ref):
    places, slots = tables_ref.shape[0], tables_ref.shape[2] // 3
    return [
        jnp.concatenate([tables_ref[j, :, i * slots : (i + 1) * slots] for j in range(places)], axis=1)
        for i in range(3)
    ]


def table_places(tables_ref):
    high, middle, _ = (part.astype(F32) for part in table_parts(tables_ref))
    whole = high + middle
    return [whole[i : i + 1] for i in (SOURCE_PLACE, TARGET_PLACE, SOURCE_COLUMN)]


def chosen(from_place, to_place, source, target, first, count):
    mask = jnp.where((from_place == source) & (to_place == target), 1.0, 0.0)
    key = jnp.where(mask > 0.0, ranks(mask) - first, -1.0)
    rows = lax.broadcasted_iota(jnp.int32, (count, mask.shape[1]), 0).astype(F32)
    return jnp.where(rows == key, 1.0, 0.0)


def route_columns(first, place, tables_ref, count):
    places = tables_ref.shape[0]
    here = place.astype(F32)
    from_place, to_place, column_row = table_places(tables_ref)
    column_row = column_row + 1.0
    columns = []
    for j in range(places):
        there = lax.rem(place + j, places).astype(F32)
        select = chosen(from_place, to_place, here, there, first, count)
        columns.append(jnp.sum(select * column_row, axis=1, keepdims=True) - 1.0)
    return jnp.concatenate(columns, axis=0)


def longest(tables_ref):
    places = tables_ref.shape[0]
    from_place, to_place, _ = table_places(tables_ref)
    most = jnp.zeros((1, 1), F32)
    for source in range(places):
        for target in range(places):
            hit = jnp.where((from_place == float(source)) & (to_place == float(target)), 1.0, 0.0)
            most = jnp.maximum(most, jnp.sum(hit, axis=1, keepdims=True))
    return most


def pick_own(column, own_ref, outs):
    rows, (width, grains) = column.shape[0], own_ref.shape[1:]
    step, count = padded(width), outs[0].shape[0]
    lanes = lax.broadcasted_iota(jnp.int32, (rows, grains), 1).astype(F32)
    pick = jnp.where(lanes == column, 1.0, 0.0).astype(BF16)
    for out in outs:
        out[...] = jnp.zeros(out.shape, BF16)
    for c in range(3):
        found = lax.dot_general(pick, own_ref[c], NT, preferred_element_type=F32)
        for j, out in enumerate(outs):
            out[:, c * step : c * step + width] = found[j * count : (j + 1) * count].astype(BF16)


def add_listed(column, rims_ref, grains, outs):
    rows, groups, rim = column.shape[0], rims_ref.shape[0], rims_ref.shape[1]
    span, count = rims_ref.shape[2], outs[0].shape[0]
    lanes = lax.broadcasted_iota(jnp.int32, (rows, groups * rim), 1).astype(F32) + float(grains)
    pick = jnp.where(lanes == column, 1.0, 0.0).astype(BF16)
    for begin in range(0, span, span // 3):
        part = slice(begin, begin + span // 3)
        rims = rims_ref[:, :, part].reshape(groups * rim, span // 3)
        found = jnp.dot(pick, rims, preferred_element_type=F32)
        for j, out in enumerate(outs):
            out[:, part] = (out[:, part].astype(F32) + found[j * count : (j + 1) * count]).astype(BF16)


def route_kernel(round_ref, place_ref, tables_ref, own_ref, rims_ref, send_ref, mine_ref):
    count = mine_ref.shape[0]
    column = route_columns((round_ref[0] * count).astype(F32), place_ref[0], tables_ref, count)
    outs = [mine_ref] + [send_ref.at[j] for j in range(send_ref.shape[0])]
    pick_own(column, own_ref, outs)
    add_listed(column, rims_ref, own_ref.shape[2], outs)


def add_pairs(table, blocks, upsample_ref, normal_ref, tangent_ref, rotated_ref, grains, tile, pause=None):
    nodes, width = upsample_ref.shape
    rows = table.shape[0]
    step = padded(width)
    frame = [table[:, i : i + 1] for i in range(9)]
    stacked = jnp.concatenate([ref[:, d * step : d * step + width] for d in range(3) for ref in blocks], axis=0)

    def evaluate(begin, size):
        found = lax.dot_general(stacked, upsample_ref[pl.ds(begin, size), :], NT, preferred_element_type=F32)
        values = [found[d * rows : (d + 1) * rows].astype(BF16).astype(F32) for d in range(3)]
        for c in range(3):
            turned = frame[3 * c] * values[0] + frame[3 * c + 1] * values[1] + frame[3 * c + 2] * values[2]
            rotated_ref[c * rows : (c + 1) * rows, pl.ds(begin, size)] = turned.astype(BF16)

    if tile >= 1024:
        for begin in range(0, nodes, tile):
            evaluate(begin, min(tile, nodes - begin))
            if pause is not None:
                pause()
    else:

        def body(i, carry):
            evaluate(pl.multiple_of(i * tile, tile), tile)
            return carry

        lax.fori_loop(0, nodes // tile, body, 0)
        if nodes % tile:
            evaluate(nodes // tile * tile, nodes % tile)
    normal = jnp.dot(rotated_ref[:rows], normal_ref[...], preferred_element_type=F32)
    tangent = jnp.dot(rotated_ref[rows : 3 * rows], tangent_ref[...], preferred_element_type=F32)
    quad = [normal, tangent[:rows], tangent[rows:]]
    scaling = table[:, SCALE : SCALE + 1]
    lanes = lax.broadcasted_iota(jnp.int32, (rows, grains), 1).astype(F32)
    spot = jnp.where(lanes == table[:, TARGET_COLUMN : TARGET_COLUMN + 1], 1.0, 0.0).astype(BF16)
    spot = jnp.concatenate([spot, spot], axis=0)
    totals = []
    for c in range(3):
        given = (frame[c] * quad[0] + frame[3 + c] * quad[1] + frame[6 + c] * quad[2]) * scaling
        top = given.astype(BF16)
        rest = (given - top.astype(F32)).astype(BF16)
        totals.append(
            lax.dot_general(jnp.concatenate([top, rest], axis=0), spot, TN, preferred_element_type=F32)
        )
    return totals


def exchange_kernel(
    n_ha, opening, tile, round_ref, tables_ref, mine_ref, send_ref, upsample_ref, normal_ref, tangent_ref, *rest
):
    if opening:
        self_ref, own_ref, *rest = rest
    sum_ref, last_ref, table_ref, near_ref, relay_ref, all_ref, rotated_ref, send_sem, recv_sem = rest
    x, y, h = lax.axis_index("gx"), lax.axis_index("gy"), lax.axis_index("ha")
    right, left = (x, y, lax.rem(h + 1, n_ha)), (x, y, lax.rem(h + n_ha - 1, n_ha))
    count = mine_ref.shape[0]
    grains = sum_ref.shape[2]
    size = relay_ref.shape[1]
    sizes = [size, size, size, count - 3 * size]
    barrier = pltpu.get_barrier_semaphore()
    for device in (right, left):
        pl.semaphore_signal(barrier, inc=1, device_id=device, device_id_type=MESH)
    pl.semaphore_wait(barrier, 2)

    def send(source, landing, device, slot):
        copy = pltpu.make_async_remote_copy(
            src_ref=source,
            dst_ref=landing,
            send_sem=send_sem.at[slot],
            recv_sem=recv_sem.at[slot],
            device_id=device,
            device_id_type=MESH,
        )
        copy.start()
        return copy

    direct = [
        send(send_ref.at[0], near_ref.at[0], right, 0),
        send(send_ref.at[2], near_ref.at[1], left, 1),
    ]
    pieces = [(0, right), (2, left), (1, right), (3, left)]
    across = [
        send(send_ref.at[1, pl.ds(i * size, sizes[i])], relay_ref.at[i, pl.ds(0, sizes[i])], device, 2 + i)
        for i, device in pieces
    ]

    first = (round_ref[0] * count).astype(F32)
    from_place, to_place, _ = table_places(tables_ref)
    parts = jnp.concatenate(table_parts(tables_ref), axis=0)
    here = h.astype(F32)
    for place, j in enumerate((0, 1, 3, 2)):
        there = lax.rem(h + n_ha - j, n_ha).astype(F32)
        select = chosen(from_place, to_place, there, here, first, count).astype(BF16)
        found = lax.dot_general(select, parts, NT, preferred_element_type=F32)
        found = found[:, :TABLE] + found[:, TABLE : 2 * TABLE] + found[:, 2 * TABLE :]
        if j == 2:
            table_ref[...] = found
        else:
            all_ref[place * count : (place + 1) * count, :] = found
    weights = (upsample_ref, normal_ref, tangent_ref, rotated_ref, grains, tile)
    totals = add_pairs(all_ref[:count, :], [mine_ref], *weights)
    for c in range(3):
        total = totals[c]
        if opening:
            total += jnp.dot(self_ref[...], own_ref[c], preferred_element_type=F32)
        sum_ref[c] = total
    for copy in direct:
        copy.wait_recv()
    onward = []

    def pause():
        for copy, (i, device) in list(zip(across, pieces))[len(onward) : len(onward) + 2]:
            copy.wait_recv()
            onward.append(
                send(relay_ref.at[i, pl.ds(0, sizes[i])], last_ref.at[pl.ds(i * size, sizes[i])], device, 6 + i)
            )

    totals = add_pairs(all_ref[count:, :], [near_ref.at[0], near_ref.at[1]], *weights, pause)
    for c in range(3):
        sum_ref[c] += totals[c]
    while len(onward) < len(pieces):
        pause()
    for copy in direct + across:
        copy.wait_send()
    for copy in onward:
        copy.wait()


def close_kernel(tile, sum_ref, last_ref, table_ref, upsample_ref, normal_ref, tangent_ref, *rest):
    *before, out_ref, rotated_ref = rest
    width, grains = sum_ref.shape[1:]
    totals = add_pairs(
        table_ref[...], [last_ref], upsample_ref, normal_ref, tangent_ref, rotated_ref, grains, tile
    )
    for c in range(3):
        total = totals[c] + sum_ref[c]
        if before:
            total += before[0][c * width : (c + 1) * width, 0, :]
        out_ref[c * width : (c + 1) * width, 0, :] = total


def shards(
    sizes,
    density,
    upsample,
    normal_kernel,
    tangent_kernel,
    self_operator,
    rim_list,
    pair_target,
    pair_source,
    pair_weight,
    pair_angles,
    live_count,
):
    places = sizes[2]
    width, grains = density.shape[1], density.shape[4]
    nodes = upsample.shape[0]
    rim = rim_list.shape[-1]
    slots = pair_source.shape[-1]
    span = 3 * padded(width)
    count = CAPACITY
    own = density.reshape(3, width, grains)
    normal, tangent = normal_kernel.T, tangent_kernel.T
    packed = pl.pallas_call(
        functools.partial(prepare_kernel, places),
        out_shape=jax.ShapeDtypeStruct((rim + TABLE, span), BF16),
        in_specs=[SMEM] + [HBM] * 6,
        out_specs=VMEM,
        scratch_shapes=[
            pltpu.VMEM((1, rim), jnp.int32),
            pltpu.VMEM((1, slots), jnp.int32),
            pltpu.VMEM((1, slots), jnp.int32),
            pltpu.VMEM((1, slots), F32),
            pltpu.VMEM((3, 1, slots), F32),
            pltpu.VMEM((3, width, grains), BF16),
            pltpu.SemaphoreType.DMA((6,)),
        ],
        compiler_params=limit(60),
        name="prepare",
    )(
        live_count.reshape(1),
        rim_list.reshape(1, rim),
        pair_target.reshape(1, slots),
        pair_source.reshape(1, slots),
        pair_weight.reshape(1, slots),
        pair_angles.reshape(3, 1, slots),
        own,
    )
    rims, tables, send, mine, most, *weights = pl.pallas_call(
        functools.partial(gather_kernel, sizes),
        out_shape=[
            jax.ShapeDtypeStruct((9, rim, span), BF16),
            jax.ShapeDtypeStruct((places, TABLE, 3 * slots), BF16),
            jax.ShapeDtypeStruct((places - 1, count, span), BF16),
            jax.ShapeDtypeStruct((count, span), BF16),
            jax.ShapeDtypeStruct((1, 128), F32),
            jax.ShapeDtypeStruct((nodes, width), BF16),
            jax.ShapeDtypeStruct((nodes, width), BF16),
            jax.ShapeDtypeStruct((nodes, width), BF16),
        ],
        in_specs=[ANY] + [HBM] * 4,
        out_specs=[VMEM] * 8,
        scratch_shapes=[
            pltpu.VMEM((3, width, grains), BF16),
            pltpu.SemaphoreType.DMA((places + 10,)),
            pltpu.SemaphoreType.DMA((places + 10,)),
            pltpu.SemaphoreType.DMA((2,)),
            pltpu.SemaphoreType.DMA((4,)),
        ],
        compiler_params=limit(24, collective_id=0, has_side_effects=True),
        name="gather",
    )(packed, own, upsample, normal, tangent)
    place = lax.axis_index("ha").astype(jnp.int32).reshape(1)

    def route(turn):
        return pl.pallas_call(
            route_kernel,
            out_shape=[
                jax.ShapeDtypeStruct((places - 1, count, span), BF16),
                jax.ShapeDtypeStruct((count, span), BF16),
            ],
            in_specs=[SMEM, SMEM, VMEM, VMEM, VMEM],
            out_specs=[VMEM, VMEM],
            compiler_params=limit(24),
            name="route",
        )(turn, place, tables, own, rims)

    def finish(turn, mine, send, before):
        opening = before is None
        tile = WIDE if opening else NARROW
        held = weights if opening else [upsample, normal, tangent]
        mixed = [self_operator, own] if opening else []
        total, last, rows = pl.pallas_call(
            functools.partial(exchange_kernel, places, opening, tile),
            out_shape=[
                jax.ShapeDtypeStruct((3, width, grains), F32),
                jax.ShapeDtypeStruct((count, span), BF16),
                jax.ShapeDtypeStruct((count, TABLE), F32),
            ],
            in_specs=[SMEM, VMEM, VMEM, ANY] + [VMEM] * (3 + len(mixed)),
            out_specs=[VMEM] * 3,
            scratch_shapes=[
                pltpu.VMEM((2, count, span), BF16),
                pltpu.VMEM((4, (count // 4 + 7) // 8 * 8, span), BF16),
                pltpu.VMEM((3 * count, TABLE), F32),
                pltpu.VMEM((6 * count, nodes), BF16),
                pltpu.SemaphoreType.DMA((10,)),
                pltpu.SemaphoreType.DMA((10,)),
            ],
            compiler_params=limit(30, collective_id=1 if opening else 2, has_side_effects=True),
            name="exchange",
        )(turn, tables, mine, send, *held, *mixed)
        ended = [] if opening else [before]
        return pl.pallas_call(
            functools.partial(close_kernel, tile),
            out_shape=jax.ShapeDtypeStruct((3 * width, 1, grains), F32),
            in_specs=[VMEM] * (6 + len(ended)),
            out_specs=VMEM,
            scratch_shapes=[pltpu.VMEM((3 * count, nodes), BF16)],
            compiler_params=limit(30),
            name="close",
        )(total, last, rows, *held, *ended)

    turn = jnp.zeros((1,), jnp.int32)
    result = finish(turn, mine, send, None)
    result, most = lax.optimization_barrier((result, most))
    rounds = (most[0, 0].astype(jnp.int32) + count - 1) // count

    def again(state):
        now, total = state
        send, mine = route(now.reshape(1))
        return now + 1, finish(now.reshape(1), mine, send, total)

    _, result = lax.while_loop(lambda state: state[0] < rounds, again, (jnp.int32(1), result))
    return result.reshape(3, width, 1, 1, grains)


def solution(mesh):
    sizes = tuple(mesh.shape[axis] for axis in ("gx", "gy", "ha"))
    return jax.shard_map(
        functools.partial(shards, sizes),
        mesh=mesh,
        in_specs=(
            P(None, None, "gx", "gy", "ha"),
            P(),
            P(),
            P(),
            P(),
            P("gx", "gy", "ha"),
            P("gx", "gy", "ha", None),
            P("gx", "gy", "ha", None),
            P("gx", "gy", "ha", None),
            P(None, "gx", "gy", "ha", None),
            P("gx", "gy", "ha"),
        ),
        out_specs=P(None, None, "gx", "gy", "ha"),
        check_vma=False,
    )
```
